32 devices in a mesh: dp: 2 (over core), tvoc: 4 (over y, x), svoc: 4 (over z).
Axes of the slice: x: 2, y: 2, z: 4, core: 2. Of those that a mesh axis runs over, the one named last changes fastest.
Arguments:
- teacher_probs: bfloat16 [256, 20480], P('dp', 'tvoc'), may hold values from 0 to 1, as said below
- block_values: bfloat16 [4, 4, 24, 128, 128], P('tvoc', 'svoc'), may hold values from 0.0099487305 to 1
- block_index: int32 [4, 4, 24, 2], P('tvoc', 'svoc'), may hold values from 0 to 39, as said below
- block_count: int32 [4, 4], P('tvoc', 'svoc'), may hold values from 5 to 24, as said below
- hidden: bfloat16 [256, 3072], P('dp'), may hold values from -48 to 48
- student_weight: bfloat16 [3072, 8192], P(None, ('tvoc', 'svoc')), may hold values from -0.15 to 0.15
Outputs:
- divergence: float32 [256], P('dp')
- grad_weight: bfloat16 [3072, 8192], P('dp', ('tvoc', 'svoc'))
- grad_hidden: float32 [256, 3072], P('dp', ('tvoc', 'svoc'))
The draws below stay inside these ranges and needn't reach their ends.
Inputs may be any that keep to these rules, and one draw needn't show every extreme that they name: `teacher_probs`: each row sums to one and every entry is positive. `block_index`: entry [i, j, s, 0] is a teacher block of shard i, entry [i, j, s, 1] is c as in the reference program. The live slots of one device name at most 2 distinct c with the same c // 4, and some value of c // 4 reaches 2 on every device. Several live slots may name the same c, with the same or another teacher block. `block_count`: the live slots are the first ones; some device has all 24 live.
All inputs are finite; a program needn't handle non-finite values.
Results may differ from the reference program's by a relative error of at most 0.013.
Values may be sent and summed in bfloat16 or wider, within the bound.
A program may use at most 64 MiB of HBM per device.

```python
import math
import jax
import jax.numpy as jnp
from jax import lax

D = 3072
BLK = 128
TVB_DEV = 40
SVB_DEV = 4
SLOTS = 24
CAP = 2
TOKENS = 256
TEACHER_VOCAB = 20480
STUDENT_VOCAB = 8192
N_TVOC = 4
N_SVOC = 4


weight_limit = 0.1484375


def index_plan(key):
    base_key = jax.random.fold_in(key, 11)
    lowest = N_TVOC * (CAP - 1) + 1
    spread = SLOTS - lowest
    pair_total = N_TVOC * CAP

    def draw_device(device_key):
        pick_key, order_key, row_key, count_key, source_key, coin_key = jax.random.split(device_key, 6)
        pick_keys = jax.random.split(pick_key, N_TVOC)
        chosen = jax.vmap(lambda single_key: jax.random.permutation(single_key, SVB_DEV)[:CAP])(pick_keys)
        order = jax.random.permutation(order_key, pair_total)
        slot_range = jnp.arange(SLOTS, dtype=jnp.int32)
        fresh = order[slot_range % pair_total]
        source = jax.random.randint(source_key, (SLOTS,), 0, lowest)
        coin = jax.random.randint(coin_key, (SLOTS,), 0, 2) == 1
        pairing = jnp.where((slot_range >= lowest) & coin, order[source], fresh)
        owner = pairing // CAP
        within = pairing % CAP
        columns = owner * SVB_DEV + chosen[owner, within]
        teacher_rows = jax.random.randint(row_key, (SLOTS,), 0, TVB_DEV)
        offset = jax.random.randint(count_key, (), 0, spread + 1)
        count = SLOTS - offset * offset // max(spread, 1)
        return (jnp.stack([teacher_rows, columns], axis=-1).astype(jnp.int32), count.astype(jnp.int32))
    device_keys = jax.random.split(base_key, N_TVOC * N_SVOC)
    indices, counts = jax.vmap(draw_device)(device_keys)
    fullest = jax.random.randint(jax.random.fold_in(base_key, 5), (), 0, N_TVOC * N_SVOC)
    counts = jnp.where(jnp.arange(N_TVOC * N_SVOC) == fullest, SLOTS, counts)
    return (indices.reshape(N_TVOC, N_SVOC, SLOTS, 2), counts.reshape(N_TVOC, N_SVOC).astype(jnp.int32))


def draw_block_index(key, part):
    return index_plan(key)[0]


def draw_block_count(key, part):
    return index_plan(key)[1]


def weight_columns(key, chosen):
    column_key = jax.random.fold_in(key, 31)

    def single(column):
        return jax.random.normal(jax.random.fold_in(column_key, column), (D,), jnp.float32)
    return jax.vmap(single)(chosen) / math.sqrt(D)


def draw_student_weight(key, part):
    columns = weight_columns(key, jnp.arange(STUDENT_VOCAB, dtype=jnp.int32))
    return jnp.clip(columns.T, -weight_limit, weight_limit).astype(jnp.bfloat16)


def draw_hidden(key, part):
    base_key = jax.random.fold_in(key, 41)
    noise_key = jax.random.fold_in(base_key, 0)
    states = jax.random.normal(noise_key, (TOKENS, D), jnp.float32)
    return jnp.clip(states, -48.0, 48.0).astype(jnp.bfloat16)


def draw_teacher_probs(key, part):
    noise_key, column_key = jax.random.split(jax.random.fold_in(key, 21), 2)
    shape = (TOKENS, TEACHER_VOCAB)
    column_bias = jax.random.normal(column_key, (1, TEACHER_VOCAB), jnp.float32)
    scores = 1.5 * jax.random.normal(noise_key, shape, jnp.float32) + column_bias
    return jax.nn.softmax(scores, axis=-1).astype(jnp.bfloat16)


def levels(stream_key, shape, cuts, least, top_value):
    level = 1.0
    for position, parts in cuts:
        steps = jax.random.uniform(jax.random.fold_in(jax.random.fold_in(stream_key, 6), position), (parts,), jnp.float32, least / len(cuts), top_value / len(cuts))
        level = level * jnp.repeat(jnp.exp(steps), shape[position] // parts).reshape((-1,) + (1,) * (len(shape) - 1 - position))
    return level


def setup_inputs(seed: int = 0) -> dict:
    streams_of = jax.random.split(jax.random.key(seed), 7)
    return {
        "teacher_probs": draw_teacher_probs(jax.random.fold_in(streams_of[6], 71), 0),
        "block_values": jnp.clip(jnp.exp(math.log(1.0) - 4.61031033 * jax.random.uniform(streams_of[1], (N_TVOC, N_SVOC, SLOTS, BLK, BLK), jnp.float32) ** levels(streams_of[1], (N_TVOC, N_SVOC, SLOTS, BLK, BLK), ((0, 4), (1, 4)), -0.2, 0.2)), 0.0099487305, 1.0).astype(jnp.bfloat16),
        "block_index": draw_block_index(jax.random.fold_in(streams_of[6], 71), 0),
        "block_count": draw_block_count(jax.random.fold_in(streams_of[6], 71), 0),
        "hidden": draw_hidden(jax.random.fold_in(streams_of[6], 71), 0),
        "student_weight": draw_student_weight(jax.random.fold_in(streams_of[6], 71), 0),
    }


def reference(teacher_probs, block_values, block_index, block_count, hidden, student_weight):
    loss_scale = 128.0
    owned = N_TVOC * SVB_DEV
    shard_width = SVB_DEV * BLK

    def device_partial(teacher_shard, student_shard):
        shard_probs = lax.dynamic_slice_in_dim(teacher_probs, teacher_shard * (TVB_DEV * BLK), TVB_DEV * BLK, 1)
        shard_probs = shard_probs.reshape(TOKENS, TVB_DEV, BLK)
        indices = block_index[teacher_shard, student_shard]
        entries = block_values[teacher_shard, student_shard]
        occupied = (jnp.arange(SLOTS, dtype=jnp.int32) < block_count[teacher_shard, student_shard]).astype(jnp.float32)
        picked = jnp.take(shard_probs, indices[:, 0], axis=1)
        mapped = jnp.einsum('tsk,skc->stc', picked.astype(jnp.float32), entries.astype(jnp.float32))
        mapped = mapped * occupied[:, None, None]
        summed = jnp.zeros((owned, TOKENS, BLK), jnp.float32).at[indices[:, 1]].add(mapped)
        rounded = lax.optimization_barrier(summed.astype(jnp.bfloat16))
        return jnp.transpose(rounded.astype(jnp.float32), (1, 0, 2))

    def per_student(student_shard):

        def accumulate(running, teacher_shard):
            return (running + device_partial(teacher_shard, student_shard), None)
        running, _ = lax.scan(accumulate, jnp.zeros((TOKENS, owned, BLK), jnp.float32), jnp.arange(N_TVOC, dtype=jnp.int32))
        return running
    stacked = lax.map(per_student, jnp.arange(N_SVOC, dtype=jnp.int32))
    stacked = stacked.reshape(N_SVOC, TOKENS, N_TVOC, shard_width)
    teacher_mass = jnp.transpose(stacked, (1, 2, 0, 3)).reshape(TOKENS, STUDENT_VOCAB)
    logits = jnp.dot(hidden.astype(jnp.float32), student_weight.astype(jnp.float32), preferred_element_type=jnp.float32)
    largest = jnp.max(logits, axis=1)
    shifted = jnp.exp(logits - largest[:, None])
    total = jnp.sum(shifted, axis=1)
    mass_sum = jnp.sum(teacher_mass, axis=1)
    target = teacher_mass / mass_sum[:, None]
    positive = target > 0
    log_target = jnp.log(jnp.where(positive, target, 1.0))
    terms = jnp.where(positive, target * log_target, 0.0) - target * (logits - largest[:, None] - jnp.log(total)[:, None])
    divergence = jnp.sum(terms, axis=1)
    logit_grad = (loss_scale * (shifted / total[:, None] - target)).astype(jnp.bfloat16)
    grad_weight = jnp.dot(hidden.T.astype(jnp.float32), logit_grad.astype(jnp.float32), preferred_element_type=jnp.float32).astype(jnp.bfloat16)
    grad_hidden = jnp.dot(logit_grad.astype(jnp.float32), student_weight.T.astype(jnp.float32), preferred_element_type=jnp.float32)
    return (divergence, grad_weight, grad_hidden)
```

```python
import functools

import jax
import jax.numpy as jnp
from jax import lax
from jax.experimental import pallas as pl
from jax.experimental.pallas import tpu as pltpu
from jax.sharding import PartitionSpec as P

loss_scale = 128.0
cap = 2
MESH = pl.DeviceIdType.MESH
f32, bf16 = jnp.float32, jnp.bfloat16


def split(n_t):
    n_lo = max(k for k in range(1, n_t + 1) if n_t % k == 0 and k * k <= n_t)
    return n_t // n_lo, n_lo


def kernel(
    n_t, n_s, blk,
    idx_hbm, cnt_hbm, teacher_hbm, values_hbm, hidden_hbm, weight_hbm,
    div_ref, gw_ref, gh_ref,
    idx_s, cnt_s, teacher, values, hidden, weight, peer_hidden, hid_t, mapped, targets, tags,
    packed, landed, mass, logits, shifted, stats, stats2, grads, grad_t, gh_t,
    own0, own1, hold0, hold1, out_a0, out_a1, rel0, rel1, out_b0, out_b1, fin0, fin1, out_z, in_z,
    load_sem, weight_sem, pair_sem, pk_send, pk_recv, st_send, st_recv, rs_send, rel_sem, fin_sem, z_recv,
):
    d, i, j = lax.axis_index("dp"), lax.axis_index("tvoc"), lax.axis_index("svoc")
    n_d = 2
    n = n_t * n_s
    n_hi, n_lo = split(n_t)
    me = i * n_s + j
    other = n_d - 1 - d
    tokens, width = hidden.shape
    shard = weight.shape[1]
    per_owner = shard // blk
    half = width // n_d
    rows = width // n
    slots = values.shape[0]

    barrier = pltpu.get_barrier_semaphore()

    def greet(q, carry):
        r = lax.rem(me + q, n)
        pl.semaphore_signal(
            barrier, inc=1, device_id={"tvoc": r // n_s, "svoc": lax.rem(r, n_s)}, device_id_type=MESH)
        return carry

    loads = [
        pltpu.make_async_copy(src, dst, load_sem.at[k])
        for k, (src, dst) in enumerate((
            (idx_hbm, idx_s), (cnt_hbm, cnt_s), (values_hbm.at[0, 0], values), (hidden_hbm, hidden)))
    ]
    parts = weight_sem.shape[0]
    depth = width // parts
    weight_loads = [
        pltpu.make_async_copy(
            weight_hbm.at[pl.ds(k * depth, depth)], weight.at[pl.ds(k * depth, depth)], weight_sem.at[k])
        for k in range(parts)
    ]
    blocks = teacher.shape[0]

    def block_start(b, carry):
        pltpu.make_async_copy(
            teacher_hbm.at[:, pl.ds(pl.multiple_of(b * blk, blk), blk)], teacher.at[b], load_sem.at[4]).start()
        return carry

    loads[0].start()
    loads[1].start()
    lax.fori_loop(1, n, greet, 0)
    pl.semaphore_signal(barrier, inc=1, device_id={"dp": other}, device_id_type=MESH)
    loads[2].start()
    lax.fori_loop(0, blocks, block_start, 0)
    loads[3].start()
    for copy in weight_loads:
        copy.start()
    loads[0].wait()
    loads[1].wait()
    lanes = targets.shape[1]
    lane = lax.broadcasted_iota(jnp.int32, (slots, lanes), 1)
    slot = lax.broadcasted_iota(jnp.int32, (slots, lanes), 0)
    column = jnp.zeros((slots, lanes), jnp.int32)
    for s in range(slots):
        column = jnp.where(slot == s, idx_s[0, 0, 1, s], column)
    hot = (column == lane) & (slot < cnt_s[0, 0])
    present = jnp.max(jnp.where(hot, 1.0, 0.0), axis=0, keepdims=True)
    r_iota = lax.broadcasted_iota(jnp.int32, (lanes, lanes), 0).astype(f32)
    c_iota = lax.broadcasted_iota(jnp.int32, (lanes, lanes), 1).astype(f32)
    r_own = jnp.floor((r_iota + 0.5) / per_owner)
    c_own = jnp.floor((c_iota + 0.5) / per_owner)
    below = jnp.where((r_own == c_own) & (r_iota < c_iota), 1.0, 0.0)
    rank = jnp.dot(jnp.broadcast_to(present, (8, lanes)), below, preferred_element_type=f32)[0:1]
    place = cap * c_own[0:1] + rank
    goal = jnp.sum(jnp.where(hot, place + 1.0, 0.0), axis=1, keepdims=True) - 1.0
    targets[...] = jnp.broadcast_to(goal, (slots, lanes))
    n_tags = n_t * cap
    t_iota = lax.broadcasted_iota(jnp.int32, (n_tags, lanes), 0).astype(f32)
    within = c_iota[0:1] - per_owner * c_own[0:1]
    tag = jnp.sum(jnp.where((present > 0.0) & (place == t_iota), within + 1.0, 0.0), axis=1, keepdims=True) - 1.0
    tag_row = lax.broadcasted_iota(jnp.int32, (n_tags, tokens), 0)
    tag_lane = lax.broadcasted_iota(jnp.int32, (n_tags, tokens), 1)
    tags[...] = jnp.sum(jnp.where(tag_row == tag_lane, jnp.broadcast_to(tag, (n_tags, tokens)), 0.0), axis=0, keepdims=True)
    loads[2].wait()
    pltpu.make_async_copy(teacher, teacher, load_sem.at[4]).wait()
    for s in range(slots):
        mapped[s] = jnp.dot(teacher[idx_s[0, 0, 0, s]], values[s], preferred_element_type=f32)
    def pack(o, weighed):
        for k in range(cap):
            t = (o * cap + k).astype(f32)
            acc = jnp.zeros((tokens, blk), f32)
            for s in range(slots):
                acc = acc + jnp.where(targets[s:s + 1, 0:blk] == t, mapped[s], 0.0)
            rounded = acc.astype(bf16)
            packed[o, :, k * blk:(k + 1) * blk] = rounded
            weighed = weighed + rounded.astype(f32)
        return weighed

    weighed = lax.fori_loop(0, n_t, pack, jnp.zeros((tokens, blk), f32))
    mass_part = jnp.sum(weighed, axis=1, keepdims=True)
    loads[3].wait()
    for k in range(parts):
        weight_loads[k].wait()
        part = jnp.dot(
            hidden[:, k * depth:(k + 1) * depth], weight[k * depth:(k + 1) * depth, :], preferred_element_type=f32)
        logits[...] = part if k == 0 else logits[...] + part
    lg = logits[...]
    top = jnp.max(lg, axis=1, keepdims=True)
    e = jnp.exp(lg - top)
    e_sum = jnp.sum(e, axis=1, keepdims=True)
    shifted[...] = e

    spot = lax.broadcasted_iota(jnp.int32, (tokens, 128), 1)

    def as_rows(columns, height):
        wide = jnp.zeros((tokens, 128), f32)
        for k, part in enumerate(columns):
            wide = jnp.where(spot == k, part, wide)
        return wide.T[0:height]

    stats[me, 0:3] = as_rows((top, e_sum, mass_part), 3)
    stats[me, 3:4] = tags[...]
    pl.semaphore_wait(barrier, n)
    def to_all(ref, send, recv_near, recv_far):
        def start(ii, jj, recv):
            pltpu.make_async_remote_copy(
                src_ref=ref.at[me], dst_ref=ref.at[me], send_sem=send, recv_sem=recv,
                device_id={"tvoc": ii, "svoc": jj}, device_id_type=MESH).start()

        def far(p, carry):
            jj = lax.rem(j + p, n_s)

            def inner(q, c):
                start(lax.rem(i + q, n_t), jj, recv_far)
                return c

            return lax.fori_loop(0, n_t, inner, carry)

        def near(q, carry):
            start(lax.rem(i + q, n_t), j, recv_near)
            return carry

        lax.fori_loop(1, n_s, far, 0)
        lax.fori_loop(1, n_t, near, 0)

    to_all(stats, st_send.at[0], st_recv.at[0], st_recv.at[1])

    def packed_copy(o, src):
        return pltpu.make_async_remote_copy(
            src_ref=packed.at[o], dst_ref=landed.at[src],
            send_sem=pk_send, recv_sem=pk_recv.at[src],
            device_id={"tvoc": o}, device_id_type=MESH)

    def pack_send(q, carry):
        packed_copy(lax.rem(i + q, n_t), i).start()
        return carry

    lax.fori_loop(1, n_t, pack_send, 0)

    def hidden_copy():
        start = pl.multiple_of(other * half, blk)
        return pltpu.make_async_remote_copy(
            src_ref=hidden.at[:, pl.ds(start, half)], dst_ref=peer_hidden,
            send_sem=pair_sem.at[0], recv_sem=pair_sem.at[1],
            device_id={"dp": other}, device_id_type=MESH)

    hidden_copy().start()
    own_at = d * half

    def turn_own(k, carry):
        at = pl.multiple_of(k * blk, blk)
        tile = hidden[:, pl.ds(pl.multiple_of(own_at + at, blk), blk)].astype(f32)
        hid_t[pl.ds(at, blk), 0:tokens] = tile.T.astype(bf16)
        return carry

    lax.fori_loop(0, half // blk, turn_own, 0)
    hidden_copy().wait_recv()

    def turn_peer(k, carry):
        at = pl.multiple_of(k * blk, blk)
        hid_t[pl.ds(at, blk), tokens:2 * tokens] = peer_hidden[:, pl.ds(at, blk)].astype(f32).T.astype(bf16)
        return carry

    lax.fori_loop(0, half // blk, turn_peer, 0)
    def block_wait(ref, count, sem):
        pltpu.make_async_copy(ref.at[pl.ds(0, count)], ref.at[pl.ds(0, count)], sem).wait()

    block_wait(stats, n_t - 1, st_recv.at[0])
    def add_mass(ref, o, first):
        row = stats[o * n_s + j, 3:4]
        seat = lax.broadcasted_iota(jnp.int32, row.shape, 1)
        which = [
            jnp.sum(jnp.where(seat == i * cap + k, row, 0.0), axis=1, keepdims=True) for k in range(cap)
        ]
        for b in range(per_owner):
            acc = jnp.zeros((tokens, blk), f32) if first else mass[:, b * blk:(b + 1) * blk]
            for k in range(cap):
                part = ref[o, :, k * blk:(k + 1) * blk].astype(f32)
                acc = acc + jnp.where(which[k] == float(b), part, 0.0)
            mass[:, b * blk:(b + 1) * blk] = acc

    add_mass(packed, i, True)

    def take_mass(q, carry):
        o = lax.rem(i + q, n_t)
        packed_copy(o, o).wait_recv()
        add_mass(landed, o, False)
        return carry

    lax.fori_loop(1, n_t, take_mass, 0)
    block_wait(stats, n - n_t, st_recv.at[1])
    st = stats[...]
    largest = jnp.max(st, axis=0)[0:1]
    scale = jnp.exp(st[:, 0:1, :] - largest[None])
    line = lax.broadcasted_iota(jnp.int32, st.shape, 1)
    sums = jnp.sum(jnp.where(line == 1, st * scale, st), axis=0)
    total, mass_sum = sums[1:2], sums[2:3]
    rows8 = lax.broadcasted_iota(jnp.int32, (128, tokens), 0)
    back = jnp.where(rows8 == 0, largest, jnp.where(rows8 == 1, loss_scale / total, loss_scale / mass_sum)).T
    factor = jnp.exp(top - back[:, 0:1]) * back[:, 1:2]
    g = shifted[...] * factor - mass[...] * back[:, 2:3]
    grads[0:tokens, :] = g.astype(bf16)
    lg_copy = pltpu.make_async_remote_copy(
        src_ref=grads.at[pl.ds(0, tokens)], dst_ref=grads.at[pl.ds(tokens, tokens)],
        send_sem=pair_sem.at[2], recv_sem=pair_sem.at[3],
        device_id={"dp": other}, device_id_type=MESH)
    lg_copy.start()
    grad_t[...] = g.T.astype(bf16)
    direct = rows % 16 == 0
    if not direct:
        tile = 2 * blk

        def gh_step(k, carry):
            at = pl.multiple_of(k * tile, tile)
            gh_t[pl.ds(at, tile), :] = jnp.dot(weight[pl.ds(at, tile), :], grad_t[...], preferred_element_type=f32)
            return carry

        lax.fori_loop(0, width // tile, gh_step, 0)

    def chunk(ii, jj):
        start = (ii * n_s + jj) * rows
        if not direct:
            return gh_t[pl.ds(pl.multiple_of(start, 8), rows), :]
        return jnp.dot(weight[pl.ds(pl.multiple_of(start, 16), rows), :], grad_t[...], preferred_element_type=f32)

    hi, lo = i // n_lo, lax.rem(i, n_lo)
    sizes = ((n_lo, n_hi), (n_hi, n_lo))
    cut = own0.shape[1]
    own, hold = (own0, own1), (hold0, hold1)
    out_a, rel = (out_a0, out_a1), (rel0, rel1)
    out_b, fin = (out_b0, out_b1), (fin0, fin1)

    def at_lo(q):
        return hi * n_lo + lax.rem(lo + q, n_lo)

    def at_hi(r):
        return lax.rem(hi + r, n_hi) * n_lo + lo

    def first(h, q):
        return at_lo(q) if h == 0 else at_hi(q)

    def second(h, r):
        return at_hi(r) if h == 0 else at_lo(r)

    def order(p):
        if p == n_s - 1:
            return j
        above = n_s - 1 - j
        low = jnp.where(p < above, n_s - 1 - p, p - above)
        high = jnp.where(p < j, p, n_s - 1 - (p - j))
        return jnp.where(2 * j < n_s, low, high)

    def relay_in(h, p, q, r):
        return pltpu.make_async_remote_copy(
            src_ref=out_a[h].at[p, q - 1, r], dst_ref=rel[h].at[p, q - 1, r - 1],
            send_sem=rs_send.at[h], recv_sem=rel_sem.at[h, p],
            device_id={"tvoc": first(h, q)}, device_id_type=MESH)

    def keep_in(h, p, q):
        return pltpu.make_async_remote_copy(
            src_ref=out_a[h].at[p, q - 1, 0], dst_ref=fin[h].at[p, q - 1],
            send_sem=rs_send.at[h], recv_sem=fin_sem.at[h, p],
            device_id={"tvoc": first(h, q)}, device_id_type=MESH)

    def relay_out(h, p, r):
        return pltpu.make_async_remote_copy(
            src_ref=out_b[h].at[p, r - 1], dst_ref=fin[h].at[p, sizes[h][0] - 2 + r],
            send_sem=rs_send.at[2 + h], recv_sem=fin_sem.at[h, p],
            device_id={"tvoc": second(h, r)}, device_id_type=MESH)

    def whole_wait(ref, sem):
        pltpu.make_async_copy(ref, ref, sem).wait()

    def dots(p):
        jj = order(p)
        for q in reversed(range(n_lo)):
            for r in reversed(range(n_hi)):
                ii = lax.rem(hi + r, n_hi) * n_lo + lax.rem(lo + q, n_lo)
                both = chunk(ii, jj)
                for h, (a, b) in enumerate(((q, r), (r, q))):
                    value = both[0:cut] if h == 0 else both[cut:]
                    if a:
                        out_a[h][p, a - 1, b] = value.astype(bf16)
                        (relay_in(h, p, a, b) if b else keep_in(h, p, a)).start()
                    elif b:
                        hold[h][p, b - 1] = value
                    else:
                        own[h][p] = value

    def relay(p):
        for h in range(2):
            n_a, n_b = sizes[h]
            if n_a == 1 or n_b == 1:
                if n_b > 1:
                    for r in range(1, n_b):
                        out_b[h][p, r - 1] = hold[h][p, r - 1].astype(bf16)
                        relay_out(h, p, r).start()
                continue
            whole_wait(rel[h].at[p], rel_sem.at[h, p])
            for r in range(1, n_b):
                acc = hold[h][p, r - 1]
                for q in range(1, n_a):
                    acc = acc + rel[h][p, q - 1, r - 1].astype(f32)
                out_b[h][p, r - 1] = acc.astype(bf16)
                relay_out(h, p, r).start()

    def gather(p, h):
        whole_wait(fin[h].at[p], fin_sem.at[h, p])
        acc = own[h][p]
        for k in range(fin[h].shape[1]):
            acc = acc + fin[h][p, k].astype(f32)
        return acc

    def finish(p):
        jj = order(p)
        out_z[p, 0:cut] = gather(p, 0).astype(bf16)
        out_z[p, cut:] = gather(p, 1).astype(bf16)
        pltpu.make_async_remote_copy(
            src_ref=out_z.at[p], dst_ref=in_z.at[lax.rem(j - jj + n_s, n_s) - 1],
            send_sem=rs_send.at[4], recv_sem=z_recv,
            device_id={"svoc": jj}, device_id_type=MESH).start()

    tall = 2 * blk
    tiles = half // tall
    done = [0]

    def gw_step(k, carry):
        at = pl.multiple_of(k * tall, tall)
        gw_ref[pl.ds(at, tall), :] = jnp.dot(
            hid_t[pl.ds(at, tall), :], grads[...], preferred_element_type=f32).astype(bf16)
        return carry

    def fill(count):
        until = min(tiles, done[0] + count)
        lax.fori_loop(done[0], until, gw_step, 0)
        done[0] = until

    for p in range(n_s):
        dots(p)
        if p >= 1 and p < n_s - 1:
            relay(p - 1)
    tm = mass[...]
    positive = tm > 0
    stats2[me] = as_rows((
        jnp.sum(jnp.where(positive, tm * jnp.log(jnp.where(positive, tm, 1.0)), 0.0), axis=1, keepdims=True),
        jnp.sum(tm * logits[...], axis=1, keepdims=True)), 2)
    to_all(stats2, st_send.at[1], st_recv.at[2], st_recv.at[2])
    for p in range(n_s - 3):
        finish(p)
    if n_s >= 2:
        relay(n_s - 2)
    lg_copy.wait_recv()
    fill(2)
    if n_s >= 3:
        finish(n_s - 3)
    relay(n_s - 1)
    fill(2)
    if n_s >= 2:
        finish(n_s - 2)
    fill(tiles)
    block_wait(stats2, n - 1, st_recv.at[2])
    late = jnp.sum(stats2[...], axis=0)
    entropy, cross = late[0:1], late[1:2]
    div_ref[...] = entropy / mass_sum - jnp.log(mass_sum) - cross / mass_sum + largest + jnp.log(total)
    mine = [gather(n_s - 1, h) for h in range(2)]
    whole_wait(in_z, z_recv)
    for h, (start, stop) in enumerate(((0, cut), (cut, rows))):
        acc = mine[h]
        for k in range(n_s - 1):
            acc = acc + in_z[k, start:stop].astype(f32)
        gh_ref[start:stop] = acc
    hidden_copy().wait_send()
    lg_copy.wait_send()
    block_wait(packed, n_t - 1, pk_send)
    block_wait(stats, n - 1, st_send.at[0])
    block_wait(stats2, n - 1, st_send.at[1])
    for h in range(2):
        whole_wait(out_a[h], rs_send.at[h])
        whole_wait(out_b[h], rs_send.at[2 + h])
    whole_wait(out_z, rs_send.at[4])


def flush(div, gw, gh, div_out, gw_out, gh_out, sem):
    copies = [
        pltpu.make_async_copy(src, dst, sem.at[k])
        for k, (src, dst) in enumerate(((gw, gw_out), (gh, gh_out), (div, div_out)))
    ]
    for copy in copies:
        copy.start()
    for copy in copies:
        copy.wait()


def local(n_t, n_s, teacher_probs, block_values, block_index, block_count, hidden, student_weight):
    tokens, width = hidden.shape
    slots, blk = block_values.shape[2], block_values.shape[3]
    shard = student_weight.shape[1]
    half, rows, n = width // 2, width // (n_t * n_s), n_t * n_s
    n_hi, n_lo = split(n_t)
    direct = rows % 16 == 0
    cut = -(-(rows // 2) // 16) * 16
    cuts = (cut, rows - cut)
    sizes = ((n_lo, n_hi), (n_hi, n_lo))
    lanes = -(-(n_t * (shard // blk)) // 128) * 128
    vmem = pl.BlockSpec(memory_space=pltpu.VMEM)
    hbm = pl.BlockSpec(memory_space=pltpu.HBM)
    DMA = pltpu.SemaphoreType.DMA
    parcel = (n_t, tokens, cap * blk)
    V = pltpu.VMEM
    relays = [
        *(V((n_s, c, tokens), f32) for c in cuts),
        *(V((n_s, b - 1, c, tokens), f32) for c, (a, b) in zip(cuts, sizes)),
        *(V((n_s, a - 1, b, c, tokens), bf16) for c, (a, b) in zip(cuts, sizes)),
        *(V((n_s, a - 1, b - 1, c, tokens), bf16) for c, (a, b) in zip(cuts, sizes)),
        *(V((n_s, b - 1, c, tokens), bf16) for c, (a, b) in zip(cuts, sizes)),
        *(V((n_s, a + b - 2, c, tokens), bf16) for c, (a, b) in zip(cuts, sizes)),
        V((n_s - 1, rows, tokens), bf16),
        V((n_s - 1, rows, tokens), bf16),
    ]
    parts = 3 if width % (3 * 128) == 0 else 1
    div, gw, gh = pl.pallas_call(
        functools.partial(kernel, n_t, n_s, blk),
        out_shape=(
            jax.ShapeDtypeStruct((1, tokens), f32),
            jax.ShapeDtypeStruct((half, shard), bf16),
            jax.ShapeDtypeStruct((rows, tokens), f32),
        ),
        in_specs=[hbm] * 6,
        out_specs=(vmem, vmem, vmem),
        scratch_shapes=[
            pltpu.SMEM((1, 1, 2, slots), jnp.int32),
            pltpu.SMEM((1, 1), jnp.int32),
            V((teacher_probs.shape[1] // blk, tokens, blk), bf16),
            V(block_values.shape[2:], bf16),
            V(hidden.shape, bf16),
            V(student_weight.shape, bf16),
            V((tokens, half), bf16),
            V((half, 2 * tokens), bf16),
            V((slots, tokens, blk), f32),
            V((slots, lanes), f32),
            V((1, tokens), f32),
            V(parcel, bf16),
            V(parcel, bf16),
            V((tokens, shard), f32),
            V((tokens, shard), f32),
            V((tokens, shard), f32),
            V((n, 4, tokens), f32),
            V((n, 2, tokens), f32),
            V((2 * tokens, shard), bf16),
            V((shard, tokens), bf16),
            V((8, 128) if direct else (width, tokens), f32),
            *relays,
            DMA((5,)), DMA((parts,)), DMA((4,)), DMA, DMA((n_t,)), DMA((2,)), DMA((3,)),
            DMA((5,)), DMA((2, n_s)), DMA((2, n_s)), DMA,
        ],
        compiler_params=pltpu.CompilerParams(
            collective_id=0, has_side_effects=True, vmem_limit_bytes=32 * 1024 * 1024),
    )(
        pltpu.with_memory_space_constraint(jnp.swapaxes(block_index, 2, 3), pltpu.HBM), block_count,
        *(pltpu.with_memory_space_constraint(x, pltpu.HBM) for x in (teacher_probs, block_values, hidden, student_weight)))
    div, gw, gh = pl.pallas_call(
        flush,
        out_shape=tuple(jax.ShapeDtypeStruct(x.shape, x.dtype) for x in (div, gw, gh)),
        in_specs=[vmem] * 3,
        out_specs=(hbm,) * 3,
        scratch_shapes=[DMA((3,))],
        compiler_params=pltpu.CompilerParams(vmem_limit_bytes=2**20),
    )(div, gw, gh)
    return div.reshape(tokens), gw, gh.T


def solution(mesh):
    return jax.shard_map(
        functools.partial(local, mesh.shape["tvoc"], mesh.shape["svoc"]),
        mesh=mesh,
        in_specs=(
            P("dp", "tvoc"),
            P("tvoc", "svoc", None, None, None),
            P("tvoc", "svoc", None, None),
            P("tvoc", "svoc"),
            P("dp", None),
            P(None, ("tvoc", "svoc")),
        ),
        out_specs=(P("dp"), P("dp", ("tvoc", "svoc")), P("dp", ("tvoc", "svoc"))),
        check_vma=False,
    )
```

```python
import functools

import jax
import jax.numpy as jnp
from jax import lax
from jax.experimental import pallas as pl
from jax.experimental.pallas import tpu as pltpu
from jax.sharding import PartitionSpec as P

loss_scale = 128.0
cap = 2
MESH = pl.DeviceIdType.MESH
f32, bf16 = jnp.float32, jnp.bfloat16


def split(n_t):
    n_lo = max(k for k in range(1, n_t + 1) if n_t % k == 0 and k * k <= n_t)
    return n_t // n_lo, n_lo


def kernel(
    n_t, n_s, blk,
    idx_hbm, cnt_hbm, teacher_hbm, values_hbm, hidden_hbm, weight_hbm,
    div_ref, gw_ref, gh_ref,
    idx_s, cnt_s, teacher, values, hidden, weight, peer_hidden, hid_t, mapped, keeps, tags, plan, plan_s,
    packed, landed, mass, logits, shifted, stats, stats2, grads, grad_t, gh_t,
    own, own_mate, hold, out, out_pair, out_mate, fin, fin_mate, in_z, in_pair, in_mate,
    load_sem, weight_sem, pair_sem, pk_send, pk_recv, st_send, st_recv, rs_send, fin_sem, z_recv, pair_recv, mate_recv,
):
    d, i, j = lax.axis_index("dp"), lax.axis_index("tvoc"), lax.axis_index("svoc")
    n_d = 2
    n = n_t * n_s
    n_hi, n_lo = split(n_t)
    me = i * n_s + j
    other = n_d - 1 - d
    tokens, width = hidden.shape
    shard = weight.shape[1]
    per_owner = shard // blk
    half = width // n_d
    rows = width // n
    slots = values.shape[0]

    barrier = pltpu.get_barrier_semaphore()

    def greet(q, carry):
        r = lax.rem(me + q, n)
        pl.semaphore_signal(
            barrier, inc=1, device_id={"tvoc": r // n_s, "svoc": lax.rem(r, n_s)}, device_id_type=MESH)
        return carry

    loads = [
        pltpu.make_async_copy(src, dst, load_sem.at[k])
        for k, (src, dst) in enumerate((
            (idx_hbm, idx_s), (cnt_hbm, cnt_s), (values_hbm.at[0, 0], values), (hidden_hbm, hidden)))
    ]
    parts = weight_sem.shape[0]
    depth = width // parts
    weight_loads = [
        pltpu.make_async_copy(
            weight_hbm.at[pl.ds(k * depth, depth)], weight.at[pl.ds(k * depth, depth)], weight_sem.at[k])
        for k in range(parts)
    ]
    blocks = teacher.shape[0]

    def block_start(b, carry):
        pltpu.make_async_copy(
            teacher_hbm.at[:, pl.ds(pl.multiple_of(b * blk, blk), blk)], teacher.at[b], load_sem.at[4]).start()
        return carry

    loads[2].start()
    loads[0].start()
    loads[1].start()
    loads[3].start()
    lax.fori_loop(1, n, greet, 0)
    pl.semaphore_signal(barrier, inc=1, device_id={"dp": other}, device_id_type=MESH)
    lax.fori_loop(0, blocks, block_start, 0)
    for copy in weight_loads:
        copy.start()
    loads[0].wait()
    loads[1].wait()
    lanes = keeps.shape[1]
    lane = lax.broadcasted_iota(jnp.int32, (slots, lanes), 1)
    slot = lax.broadcasted_iota(jnp.int32, (slots, lanes), 0)
    column = jnp.zeros((slots, lanes), jnp.int32)
    for s in range(slots):
        column = jnp.where(slot == s, idx_s[0, 0, 1, s], column)
    live = slot < cnt_s[0, 0]
    hot = (column == lane) & live
    present = jnp.max(jnp.where(hot, 1.0, 0.0), axis=0, keepdims=True)
    r_iota = lax.broadcasted_iota(jnp.int32, (lanes, lanes), 0).astype(f32)
    c_iota = lax.broadcasted_iota(jnp.int32, (lanes, lanes), 1).astype(f32)
    r_own = jnp.floor((r_iota + 0.5) / per_owner)
    c_own = jnp.floor((c_iota + 0.5) / per_owner)
    below = jnp.where((r_own == c_own) & (r_iota < c_iota), 1.0, 0.0)
    rank = jnp.dot(jnp.broadcast_to(present, (8, lanes)), below, preferred_element_type=f32)[0:1]
    place = cap * c_own[0:1] + rank
    n_tags = n_t * cap
    t_iota = lax.broadcasted_iota(jnp.int32, (n_tags, lanes), 0).astype(f32)
    within = c_iota[0:1] - per_owner * c_own[0:1]
    named = (present > 0.0) & (place == t_iota)
    tag_diag = lax.broadcasted_iota(jnp.int32, (n_tags, lanes), 0) == lax.broadcasted_iota(jnp.int32, (n_tags, lanes), 1)

    def along(col):
        return jnp.sum(jnp.where(tag_diag, jnp.broadcast_to(col, (n_tags, lanes)), 0.0), axis=0, keepdims=True)

    tags[...] = along(jnp.sum(jnp.where(named, within + 1.0, 0.0), axis=1, keepdims=True) - 1.0)[:, 0:tokens]
    upto = jnp.sum(jnp.where(live & (column <= lane), 1.0, 0.0), axis=0, keepdims=True)
    last = jnp.sum(jnp.where(named, upto, 0.0), axis=1, keepdims=True)
    last = jnp.where(last > 0.0, last - 1.0, float(slots))
    slot_f, lane_f = slot.astype(f32), lane.astype(f32)
    diag = slot == lane
    key = jnp.where(live, column * slots, lanes * slots).astype(f32) + slot_f
    key_row = jnp.sum(jnp.where(diag, key, 0.0), axis=0, keepdims=True)
    key_row = jnp.where(lane_f[0:1] < slots, key_row, 2.0 * lanes * slots)
    spot_of = jnp.sum(jnp.where(key_row < key, 1.0, 0.0), axis=1, keepdims=True)
    here = spot_of == lane_f
    plan[0:1] = jnp.sum(jnp.where(here, slot_f, 0.0), axis=0, keepdims=True).astype(jnp.int32)
    plan[1:2] = along(last).astype(jnp.int32)
    plan_copy = pltpu.make_async_copy(plan, plan_s, load_sem.at[5])
    plan_copy.start()
    sorted_row = jnp.sum(jnp.where(here, column.astype(f32), 0.0), axis=0, keepdims=True)
    same = jnp.where(sorted_row == pltpu.roll(sorted_row, 1, 1), 1.0, 0.0)
    keeps[...] = jnp.broadcast_to(jnp.sum(jnp.where(diag, same, 0.0), axis=1, keepdims=True), (slots, lanes))
    mapped[slots] = jnp.zeros((tokens, blk), f32)
    plan_copy.wait()
    loads[2].wait()
    pltpu.make_async_copy(teacher, teacher, load_sem.at[4]).wait()
    run = None
    for k in range(slots):
        s = jnp.clip(plan_s[0, k], 0, slots - 1)
        term = jnp.dot(teacher[idx_s[0, 0, 0, s]], values[s], preferred_element_type=f32)
        run = term if k == 0 else term + keeps[k:k + 1, 0:blk] * run
        mapped[k] = run
    def pack(o, weighed):
        for k in range(cap):
            rounded = mapped[jnp.clip(plan_s[1, o * cap + k], 0, slots)].astype(bf16)
            packed[o, :, k * blk:(k + 1) * blk] = rounded
            weighed = weighed + rounded.astype(f32)
        return weighed

    weighed = lax.fori_loop(0, n_t, pack, jnp.zeros((tokens, blk), f32))
    mass_part = jnp.sum(weighed, axis=1, keepdims=True)
    loads[3].wait()
    for k in range(parts):
        weight_loads[k].wait()
        part = jnp.dot(
            hidden[:, k * depth:(k + 1) * depth], weight[k * depth:(k + 1) * depth, :], preferred_element_type=f32)
        logits[...] = part if k == 0 else logits[...] + part
    lg = logits[...]
    top = jnp.max(lg, axis=1, keepdims=True)
    e = jnp.exp(lg - top)
    e_sum = jnp.sum(e, axis=1, keepdims=True)
    shifted[...] = e

    spot = lax.broadcasted_iota(jnp.int32, (tokens, 128), 1)

    def as_rows(columns, height):
        wide = jnp.zeros((tokens, 128), f32)
        for k, part in enumerate(columns):
            wide = jnp.where(spot == k, part, wide)
        return wide.T[0:height]

    stats[me, 0:3] = as_rows((top, e_sum, mass_part), 3)
    stats[me, 3:4] = tags[...]
    pl.semaphore_wait(barrier, n)
    def to_all(ref, send, recv_near, recv_far):
        def start(ii, jj, recv):
            pltpu.make_async_remote_copy(
                src_ref=ref.at[me], dst_ref=ref.at[me], send_sem=send, recv_sem=recv,
                device_id={"tvoc": ii, "svoc": jj}, device_id_type=MESH).start()

        def far(p, carry):
            jj = lax.rem(j + p, n_s)

            def inner(q, c):
                start(lax.rem(i + q, n_t), jj, recv_far)
                return c

            return lax.fori_loop(0, n_t, inner, carry)

        def near(q, carry):
            start(lax.rem(i + q, n_t), j, recv_near)
            return carry

        lax.fori_loop(1, n_s, far, 0)
        lax.fori_loop(1, n_t, near, 0)

    to_all(stats, st_send.at[0], st_recv.at[0], st_recv.at[1])

    def spread(k):
        return lax.rem(i // n_lo + lax.rem(k, n_hi), n_hi) * n_lo + lax.rem(i + k // n_hi, n_lo)

    def packed_copy(o, src):
        return pltpu.make_async_remote_copy(
            src_ref=packed.at[o], dst_ref=landed.at[src],
            send_sem=pk_send, recv_sem=pk_recv.at[src],
            device_id={"tvoc": o}, device_id_type=MESH)

    def pack_send(q, carry):
        packed_copy(spread(n_t - q), i).start()
        return carry

    lax.fori_loop(1, n_t, pack_send, 0)

    def hidden_copy():
        start = pl.multiple_of(other * half, blk)
        return pltpu.make_async_remote_copy(
            src_ref=hidden.at[:, pl.ds(start, half)], dst_ref=peer_hidden,
            send_sem=pair_sem.at[0], recv_sem=pair_sem.at[1],
            device_id={"dp": other}, device_id_type=MESH)

    hidden_copy().start()
    own_at = d * half

    def turn_own(k, carry):
        at = pl.multiple_of(k * blk, blk)
        tile = hidden[:, pl.ds(pl.multiple_of(own_at + at, blk), blk)].astype(f32)
        hid_t[pl.ds(at, blk), 0:tokens] = tile.T.astype(bf16)
        return carry

    lax.fori_loop(0, half // blk, turn_own, 0)
    hidden_copy().wait_recv()

    def turn_peer(k, carry):
        at = pl.multiple_of(k * blk, blk)
        hid_t[pl.ds(at, blk), tokens:2 * tokens] = peer_hidden[:, pl.ds(at, blk)].astype(f32).T.astype(bf16)
        return carry

    lax.fori_loop(0, half // blk, turn_peer, 0)
    def block_wait(ref, count, sem):
        pltpu.make_async_copy(ref.at[pl.ds(0, count)], ref.at[pl.ds(0, count)], sem).wait()

    block_wait(stats, n_t - 1, st_recv.at[0])
    def add_mass(ref, o, first):
        row = stats[o * n_s + j, 3:4]
        seat = lax.broadcasted_iota(jnp.int32, row.shape, 1)
        which = [
            jnp.sum(jnp.where(seat == i * cap + k, row, 0.0), axis=1, keepdims=True) for k in range(cap)
        ]
        for b in range(per_owner):
            acc = jnp.zeros((tokens, blk), f32) if first else mass[:, b * blk:(b + 1) * blk]
            for k in range(cap):
                part = ref[o, :, k * blk:(k + 1) * blk].astype(f32)
                acc = acc + jnp.where(which[k] == float(b), part, 0.0)
            mass[:, b * blk:(b + 1) * blk] = acc

    add_mass(packed, i, True)

    def take_mass(q, carry):
        o = spread(q)
        packed_copy(o, o).wait_recv()
        add_mass(landed, o, False)
        return carry

    lax.fori_loop(1, n_t, take_mass, 0)
    block_wait(stats, n - n_t, st_recv.at[1])
    st = stats[...]
    largest = jnp.max(st, axis=0)[0:1]
    scale = jnp.exp(st[:, 0:1, :] - largest[None])
    line = lax.broadcasted_iota(jnp.int32, st.shape, 1)
    sums = jnp.sum(jnp.where(line == 1, st * scale, st), axis=0)
    total, mass_sum = sums[1:2], sums[2:3]
    rows8 = lax.broadcasted_iota(jnp.int32, (128, tokens), 0)
    back = jnp.where(rows8 == 0, largest, jnp.where(rows8 == 1, loss_scale / total, loss_scale / mass_sum)).T
    factor = jnp.exp(top - back[:, 0:1]) * back[:, 1:2]
    g = shifted[...] * factor - mass[...] * back[:, 2:3]
    grads[0:tokens, :] = g.astype(bf16)
    lg_copy = pltpu.make_async_remote_copy(
        src_ref=grads.at[pl.ds(0, tokens)], dst_ref=grads.at[pl.ds(tokens, tokens)],
        send_sem=pair_sem.at[2], recv_sem=pair_sem.at[3],
        device_id={"dp": other}, device_id_type=MESH)
    lg_copy.start()
    grad_t[...] = g.T.astype(bf16)
    direct = rows % 16 == 0
    if not direct:
        tile = 2 * blk

        def gh_step(k, carry):
            at = pl.multiple_of(k * tile, tile)
            gh_t[pl.ds(at, tile), :] = jnp.dot(weight[pl.ds(at, tile), :], grad_t[...], preferred_element_type=f32)
            return carry

        lax.fori_loop(0, width // tile, gh_step, 0)

    def chunk(ii, jj, begin=0, end=rows):
        start = (ii * n_s + jj) * rows + begin
        if not direct:
            return gh_t[pl.ds(pl.multiple_of(start, 8), end - begin), :]
        return jnp.dot(
            weight[pl.ds(pl.multiple_of(start, 16), end - begin), :], grad_t[...], preferred_element_type=f32)

    hi, lo = i // n_lo, lax.rem(i, n_lo)
    early = in_pair.shape[1]
    rest = rows - early

    def place_of(k):
        q, r = k // n_hi, k % n_hi
        return lax.rem(hi + r, n_hi) * n_lo + lax.rem(lo + q, n_lo)

    def order(p):
        if p == n_s - 1:
            return j
        if p == n_s - 2:
            return j + 1 - 2 * lax.rem(j, 2)
        pairs, jp, pp, member = n_s // 2, j // 2, p // 2, p % 2
        above = pairs - 1 - jp
        low = 2 * jnp.where(pp < above, pairs - 1 - pp, pp - above) + 1 - member
        high = 2 * jnp.where(pp < jp, pp, pairs - 1 - (pp - jp)) + member
        return jnp.where(2 * jp < pairs, low, high)

    mate = order(n_s - 2)

    def slot_of(jj):
        return lax.rem(j // 2 - jj // 2 + n_s // 2, n_s // 2) * 2 - 2 + lax.rem(j, 2)

    def whole_wait(ref, sem):
        pltpu.make_async_copy(ref, ref, sem).wait()

    counts = [0, 0, 0]

    def ship(kind, value, dst, recv, where):
        src = (out, out_pair, out_mate)[kind].at[counts[kind]]
        counts[kind] += 1
        src[...] = value.astype(bf16)
        pltpu.make_async_remote_copy(
            src_ref=src, dst_ref=dst, send_sem=rs_send.at[kind], recv_sem=recv,
            device_id=where, device_id_type=MESH).start()

    def send_dots(p):
        for k in reversed(range(1, n_t)):
            ii = place_of(k)
            if p == n_s - 2:
                ship(2, chunk(ii, mate, early), fin_mate.at[k - 1], fin_sem.at[p], {"tvoc": ii})
            else:
                ship(0, chunk(ii, order(p)), fin.at[p, k - 1], fin_sem.at[p], {"tvoc": ii})

    def pair_dots():
        for k in reversed(range(n_t)):
            ship(1, chunk(place_of(k), mate, 0, early), in_pair.at[k], pair_recv, {"svoc": mate})

    def own_dots():
        for k in reversed(range(n_t)):
            hold[k] = chunk(place_of(k), j)

    def own_send():
        whole_wait(in_pair, pair_recv)
        for k in reversed(range(n_t)):
            hold[k, 0:early] = hold[k, 0:early] + in_pair[k].astype(f32)
            if k:
                ship(0, hold[k], fin.at[n_s - 1, k - 1], fin_sem.at[n_s - 1], {"tvoc": place_of(k)})

    def gather(p):
        if p == n_s - 2:
            acc, terms = own_mate[...], fin_mate
        else:
            acc, terms = own[p] if p < n_s - 1 else hold[0], fin.at[p]
        if n_t > 1:
            whole_wait(terms, fin_sem.at[p])
        for k in range(n_t - 1):
            acc = acc + terms[k].astype(f32)
        return acc

    def finish(p):
        jj = order(p)
        if p == n_s - 2:
            ship(2, gather(p), in_mate, mate_recv, {"svoc": jj})
        else:
            ship(0, gather(p), in_z.at[slot_of(jj)], z_recv, {"svoc": jj})

    tall = 2 * blk
    tiles = half // tall
    done = [0]

    def gw_step(k, carry):
        at = pl.multiple_of(k * tall, tall)
        gw_ref[pl.ds(at, tall), :] = jnp.dot(
            hid_t[pl.ds(at, tall), :], grads[...], preferred_element_type=f32).astype(bf16)
        return carry

    def fill(count):
        until = min(tiles, done[0] + count)
        lax.fori_loop(done[0], until, gw_step, 0)
        done[0] = until

    def spread_late():
        tm = mass[...]
        positive = tm > 0
        stats2[me] = as_rows((
            jnp.sum(jnp.where(positive, tm * jnp.log(jnp.where(positive, tm, 1.0)), 0.0), axis=1, keepdims=True),
            jnp.sum(tm * logits[...], axis=1, keepdims=True)), 2)
        to_all(stats2, st_send.at[1], st_recv.at[2], st_recv.at[2])

    for p in range(n_s - 2):
        send_dots(p)
        if p == 0:
            pair_dots()
    if n_s == 2:
        pair_dots()
    send_dots(n_s - 2)
    for p in range(n_s - 2):
        own[p] = chunk(i, order(p))
    own_mate[...] = chunk(i, mate, early)
    own_dots()
    spread_late()
    lg_copy.wait_recv()
    fill(tiles)
    own_send()
    for p in range(n_s - 1):
        finish(p)
    block_wait(stats2, n - 1, st_recv.at[2])
    late = jnp.sum(stats2[...], axis=0)
    entropy, cross = late[0:1], late[1:2]
    div_ref[...] = entropy / mass_sum - jnp.log(mass_sum) - cross / mass_sum + largest + jnp.log(total)
    acc = gather(n_s - 1)
    if n_s > 2:
        whole_wait(in_z, z_recv)
    for k in range(n_s - 2):
        acc = acc + in_z[k].astype(f32)
    gh_ref[0:early] = acc[0:early]
    whole_wait(in_mate, mate_recv)
    gh_ref[early:] = acc[early:] + in_mate[...].astype(f32)
    hidden_copy().wait_send()
    lg_copy.wait_send()
    block_wait(packed, n_t - 1, pk_send)
    block_wait(stats, n - 1, st_send.at[0])
    block_wait(stats2, n - 1, st_send.at[1])
    for kind, ref in enumerate((out, out_pair, out_mate)):
        block_wait(ref, counts[kind], rs_send.at[kind])


def flush(div, gw, gh, div_out, gw_out, gh_out, sem):
    copies = [
        pltpu.make_async_copy(src, dst, sem.at[k])
        for k, (src, dst) in enumerate(((gw, gw_out), (gh, gh_out), (div, div_out)))
    ]
    for copy in copies:
        copy.start()
    for copy in copies:
        copy.wait()


def local(n_t, n_s, teacher_probs, block_values, block_index, block_count, hidden, student_weight):
    tokens, width = hidden.shape
    slots, blk = block_values.shape[2], block_values.shape[3]
    shard = student_weight.shape[1]
    half, rows, n = width // 2, width // (n_t * n_s), n_t * n_s
    n_hi, n_lo = split(n_t)
    direct = rows % 16 == 0
    lanes = -(-(n_t * (shard // blk)) // 128) * 128
    vmem = pl.BlockSpec(memory_space=pltpu.VMEM)
    hbm = pl.BlockSpec(memory_space=pltpu.HBM)
    DMA = pltpu.SemaphoreType.DMA
    parcel = (n_t, tokens, cap * blk)
    V = pltpu.VMEM
    early = -(-(rows // 2) // 16) * 16
    rest = rows - early
    exchange = [
        V((n_s - 1, rows, tokens), f32),
        V((rest, tokens), f32),
        V((n_t, rows, tokens), f32),
        V((n_s * n_t, rows, tokens), bf16),
        V((n_t, early, tokens), bf16),
        V((n_t, rest, tokens), bf16),
        V((n_s, n_t - 1, rows, tokens), bf16),
        V((n_t - 1, rest, tokens), bf16),
        V((max(n_s - 2, 1), rows, tokens), bf16),
        V((n_t, early, tokens), bf16),
        V((rest, tokens), bf16),
    ]
    parts = 3 if width % (3 * 128) == 0 else 1
    div, gw, gh = pl.pallas_call(
        functools.partial(kernel, n_t, n_s, blk),
        out_shape=(
            jax.ShapeDtypeStruct((1, tokens), f32),
            jax.ShapeDtypeStruct((half, shard), bf16),
            jax.ShapeDtypeStruct((rows, tokens), f32),
        ),
        in_specs=[hbm] * 6,
        out_specs=(vmem, vmem, vmem),
        scratch_shapes=[
            pltpu.SMEM((1, 1, 2, slots), jnp.int32),
            pltpu.SMEM((1, 1), jnp.int32),
            V((teacher_probs.shape[1] // blk, tokens, blk), bf16),
            V(block_values.shape[2:], bf16),
            V(hidden.shape, bf16),
            V(student_weight.shape, bf16),
            V((tokens, half), bf16),
            V((half, 2 * tokens), bf16),
            V((slots + 1, tokens, blk), f32),
            V((slots, lanes), f32),
            V((1, tokens), f32),
            V((2, lanes), jnp.int32),
            pltpu.SMEM((2, lanes), jnp.int32),
            V(parcel, bf16),
            V(parcel, bf16),
            V((tokens, shard), f32),
            V((tokens, shard), f32),
            V((tokens, shard), f32),
            V((n, 4, tokens), f32),
            V((n, 2, tokens), f32),
            V((2 * tokens, shard), bf16),
            V((shard, tokens), bf16),
            V((8, 128) if direct else (width, tokens), f32),
            *exchange,
            DMA((6,)), DMA((parts,)), DMA((4,)), DMA, DMA((n_t,)), DMA((2,)), DMA((3,)),
            DMA((3,)), DMA((n_s,)), DMA, DMA, DMA,
        ],
        compiler_params=pltpu.CompilerParams(
            collective_id=0, has_side_effects=True, vmem_limit_bytes=32 * 1024 * 1024),
    )(
        pltpu.with_memory_space_constraint(jnp.swapaxes(block_index, 2, 3), pltpu.HBM), block_count,
        *(pltpu.with_memory_space_constraint(x, pltpu.HBM) for x in (teacher_probs, block_values, hidden, student_weight)))
    div, gw, gh = pl.pallas_call(
        flush,
        out_shape=tuple(jax.ShapeDtypeStruct(x.shape, x.dtype) for x in (div, gw, gh)),
        in_specs=[vmem] * 3,
        out_specs=(hbm,) * 3,
        scratch_shapes=[DMA((3,))],
        compiler_params=pltpu.CompilerParams(vmem_limit_bytes=2**20),
    )(div, gw, gh)
    return div.reshape(tokens), gw, gh.T


def solution(mesh):
    return jax.shard_map(
        functools.partial(local, mesh.shape["tvoc"], mesh.shape["svoc"]),
        mesh=mesh,
        in_specs=(
            P("dp", "tvoc"),
            P("tvoc", "svoc", None, None, None),
            P("tvoc", "svoc", None, None),
            P("tvoc", "svoc"),
            P("dp", None),
            P(None, ("tvoc", "svoc")),
        ),
        out_specs=(P("dp"), P("dp", ("tvoc", "svoc")), P("dp", ("tvoc", "svoc"))),
        check_vma=False,
    )
```

```python
import functools

import jax
import jax.numpy as jnp
from jax import lax
from jax.experimental import pallas as pl
from jax.experimental.pallas import tpu as pltpu
from jax.sharding import PartitionSpec as P

loss_scale = 128.0
cap = 2
MESH = pl.DeviceIdType.MESH
f32, bf16 = jnp.float32, jnp.bfloat16


def split(n_t):
    n_lo = max(k for k in range(1, n_t + 1) if n_t % k == 0 and k * k <= n_t)
    return n_t // n_lo, n_lo


def kernel(
    n_t, n_s, blk,
    idx_hbm, cnt_hbm, teacher_hbm, values_hbm, hidden_hbm, weight_hbm,
    div_ref, gw_ref, gh_ref,
    idx_s, cnt_s, teacher, values, hidden, weight, peer_hidden, hid_t, mapped, keeps, tags, plan, plan_s,
    packed, landed, mass, logits, shifted, tops, stats, stats2, grads, grad_t, gh_t,
    own, own_mate, hold, out, out_pair, out_mate, fin, fin_mate, in_z, in_pair, in_mate,
    load_sem, weight_sem, pair_sem, pk_send, pk_recv, st_send, st_recv, rs_send, fin_sem, z_recv, pair_recv, mate_recv,
):
    d, i, j = lax.axis_index("dp"), lax.axis_index("tvoc"), lax.axis_index("svoc")
    n_d = 2
    n = n_t * n_s
    n_hi, n_lo = split(n_t)
    me = i * n_s + j
    other = n_d - 1 - d
    tokens, width = hidden.shape
    shard = weight.shape[1]
    per_owner = shard // blk
    half = width // n_d
    rows = width // n
    slots = values.shape[0]

    barrier = pltpu.get_barrier_semaphore()

    def greet(q, carry):
        r = lax.rem(me + q, n)
        pl.semaphore_signal(
            barrier, inc=1, device_id={"tvoc": r // n_s, "svoc": lax.rem(r, n_s)}, device_id_type=MESH)
        return carry

    loads = [
        pltpu.make_async_copy(src, dst, load_sem.at[k])
        for k, (src, dst) in enumerate((
            (idx_hbm, idx_s), (cnt_hbm, cnt_s), (values_hbm.at[0, 0], values), (hidden_hbm, hidden)))
    ]
    parts = weight_sem.shape[0]
    depth = width // parts
    weight_loads = [
        pltpu.make_async_copy(
            weight_hbm.at[pl.ds(k * depth, depth)], weight.at[pl.ds(k * depth, depth)], weight_sem.at[k])
        for k in range(parts)
    ]
    blocks = teacher.shape[0]

    def block_start(b, carry):
        pltpu.make_async_copy(
            teacher_hbm.at[:, pl.ds(pl.multiple_of(b * blk, blk), blk)], teacher.at[b], load_sem.at[4]).start()
        return carry

    loads[2].start()
    loads[0].start()
    loads[1].start()
    loads[3].start()
    lax.fori_loop(1, n, greet, 0)
    pl.semaphore_signal(barrier, inc=1, device_id={"dp": other}, device_id_type=MESH)
    lax.fori_loop(0, blocks, block_start, 0)
    for copy in weight_loads:
        copy.start()
    loads[0].wait()
    loads[1].wait()
    lanes = keeps.shape[1]
    lane = lax.broadcasted_iota(jnp.int32, (slots, lanes), 1)
    slot = lax.broadcasted_iota(jnp.int32, (slots, lanes), 0)
    column = jnp.zeros((slots, lanes), jnp.int32)
    for s in range(slots):
        column = jnp.where(slot == s, idx_s[0, 0, 1, s], column)
    live = slot < cnt_s[0, 0]
    hot = (column == lane) & live
    present = jnp.max(jnp.where(hot, 1.0, 0.0), axis=0, keepdims=True)
    r_iota = lax.broadcasted_iota(jnp.int32, (lanes, lanes), 0).astype(f32)
    c_iota = lax.broadcasted_iota(jnp.int32, (lanes, lanes), 1).astype(f32)
    r_own = jnp.floor((r_iota + 0.5) / per_owner)
    c_own = jnp.floor((c_iota + 0.5) / per_owner)
    below = jnp.where((r_own == c_own) & (r_iota < c_iota), 1.0, 0.0)
    rank = jnp.dot(jnp.broadcast_to(present, (8, lanes)), below, preferred_element_type=f32)[0:1]
    place = cap * c_own[0:1] + rank
    n_tags = n_t * cap
    t_iota = lax.broadcasted_iota(jnp.int32, (n_tags, lanes), 0).astype(f32)
    within = c_iota[0:1] - per_owner * c_own[0:1]
    named = (present > 0.0) & (place == t_iota)
    tag_diag = lax.broadcasted_iota(jnp.int32, (n_tags, lanes), 0) == lax.broadcasted_iota(jnp.int32, (n_tags, lanes), 1)

    def along(col):
        return jnp.sum(jnp.where(tag_diag, jnp.broadcast_to(col, (n_tags, lanes)), 0.0), axis=0, keepdims=True)

    tags[...] = along(jnp.sum(jnp.where(named, within + 1.0, 0.0), axis=1, keepdims=True) - 1.0)[:, 0:tokens]
    upto = jnp.sum(jnp.where(live & (column <= lane), 1.0, 0.0), axis=0, keepdims=True)
    last = jnp.sum(jnp.where(named, upto, 0.0), axis=1, keepdims=True)
    last = jnp.where(last > 0.0, last - 1.0, float(slots))
    slot_f, lane_f = slot.astype(f32), lane.astype(f32)
    diag = slot == lane
    key = jnp.where(live, column * slots, lanes * slots).astype(f32) + slot_f
    key_row = jnp.sum(jnp.where(diag, key, 0.0), axis=0, keepdims=True)
    key_row = jnp.where(lane_f[0:1] < slots, key_row, 2.0 * lanes * slots)
    spot_of = jnp.sum(jnp.where(key_row < key, 1.0, 0.0), axis=1, keepdims=True)
    here = spot_of == lane_f
    plan[0:1] = jnp.sum(jnp.where(here, slot_f, 0.0), axis=0, keepdims=True).astype(jnp.int32)
    plan[1:2] = along(last).astype(jnp.int32)
    plan_copy = pltpu.make_async_copy(plan, plan_s, load_sem.at[5])
    plan_copy.start()
    sorted_row = jnp.sum(jnp.where(here, column.astype(f32), 0.0), axis=0, keepdims=True)
    same = jnp.where(sorted_row == pltpu.roll(sorted_row, 1, 1), 1.0, 0.0)
    keeps[...] = jnp.broadcast_to(jnp.sum(jnp.where(diag, same, 0.0), axis=1, keepdims=True), (slots, lanes))
    mapped[slots] = jnp.zeros((tokens, blk), f32)
    plan_copy.wait()
    loads[2].wait()
    pltpu.make_async_copy(teacher, teacher, load_sem.at[4]).wait()
    run = None
    for k in range(slots):
        s = jnp.clip(plan_s[0, k], 0, slots - 1)
        term = jnp.dot(teacher[idx_s[0, 0, 0, s]], values[s], preferred_element_type=f32)
        run = term if k == 0 else term + keeps[k:k + 1, 0:blk] * run
        mapped[k] = run
    def pack(o, weighed):
        for k in range(cap):
            rounded = mapped[jnp.clip(plan_s[1, o * cap + k], 0, slots)].astype(bf16)
            packed[o, :, k * blk:(k + 1) * blk] = rounded
            weighed = weighed + rounded.astype(f32)
        return weighed

    weighed = lax.fori_loop(0, n_t, pack, jnp.zeros((tokens, blk), f32))
    mass_part = jnp.sum(weighed, axis=1, keepdims=True)
    spot = lax.broadcasted_iota(jnp.int32, (tokens, 128), 1)

    def as_rows(columns, height):
        wide = jnp.zeros((tokens, 128), f32)
        for k, part in enumerate(columns):
            wide = jnp.where(spot == k, part, wide)
        return wide.T[0:height]

    def softmax():
        loads[3].wait()
        for k in range(parts):
            weight_loads[k].wait()
            part = jnp.dot(
                hidden[:, k * depth:(k + 1) * depth], weight[k * depth:(k + 1) * depth, :], preferred_element_type=f32)
            logits[...] = part if k == 0 else logits[...] + part
        lg = logits[...]
        top = jnp.max(lg, axis=1, keepdims=True)
        e = jnp.exp(lg - top)
        shifted[...] = e
        tops[...] = jnp.broadcast_to(top, tops.shape)
        stats[me, 0:3] = as_rows((top, jnp.sum(e, axis=1, keepdims=True), mass_part), 3)
        stats[me, 3:4] = tags[...]

    pl.when(j == 0)(softmax)
    pl.semaphore_wait(barrier, n)
    def spread(k):
        return lax.rem(i // n_lo + lax.rem(k, n_hi), n_hi) * n_lo + lax.rem(i + k // n_hi, n_lo)

    def packed_copy(o, src):
        return pltpu.make_async_remote_copy(
            src_ref=packed.at[o], dst_ref=landed.at[src],
            send_sem=pk_send, recv_sem=pk_recv.at[src],
            device_id={"tvoc": o}, device_id_type=MESH)

    near = [k for k in range(1, n_t) if k % n_hi == 0 or k < n_hi]
    away = [k for k in range(1, n_t) if k not in near]
    for k in near:
        packed_copy(spread(k), i).start()

    pl.when(j != 0)(softmax)
    def to_all(ref, send, recv_near, recv_far):
        def start(ii, jj, recv):
            pltpu.make_async_remote_copy(
                src_ref=ref.at[me], dst_ref=ref.at[me], send_sem=send, recv_sem=recv,
                device_id={"tvoc": ii, "svoc": jj}, device_id_type=MESH).start()

        def far(p, carry):
            jj = lax.rem(j + p, n_s)

            def inner(q, c):
                start(lax.rem(i + q, n_t), jj, recv_far)
                return c

            return lax.fori_loop(0, n_t, inner, carry)

        def near(q, carry):
            start(lax.rem(i + q, n_t), j, recv_near)
            return carry

        lax.fori_loop(1, n_s, far, 0)
        lax.fori_loop(1, n_t, near, 0)

    to_all(stats, st_send.at[0], st_recv.at[0], st_recv.at[1])
    for k in away:
        packed_copy(spread(k), i).start()

    def hidden_copy():
        start = pl.multiple_of(other * half, blk)
        return pltpu.make_async_remote_copy(
            src_ref=hidden.at[:, pl.ds(start, half)], dst_ref=peer_hidden,
            send_sem=pair_sem.at[0], recv_sem=pair_sem.at[1],
            device_id={"dp": other}, device_id_type=MESH)

    hidden_copy().start()
    own_at = d * half

    def turn_own(k, carry):
        at = pl.multiple_of(k * blk, blk)
        tile = hidden[:, pl.ds(pl.multiple_of(own_at + at, blk), blk)].astype(f32)
        hid_t[pl.ds(at, blk), 0:tokens] = tile.T.astype(bf16)
        return carry

    lax.fori_loop(0, half // blk, turn_own, 0)
    hidden_copy().wait_recv()

    def turn_peer(k, carry):
        at = pl.multiple_of(k * blk, blk)
        hid_t[pl.ds(at, blk), tokens:2 * tokens] = peer_hidden[:, pl.ds(at, blk)].astype(f32).T.astype(bf16)
        return carry

    lax.fori_loop(0, half // blk, turn_peer, 0)
    def block_wait(ref, count, sem):
        pltpu.make_async_copy(ref.at[pl.ds(0, count)], ref.at[pl.ds(0, count)], sem).wait()

    block_wait(stats, n_t - 1, st_recv.at[0])
    def add_mass(ref, o, first):
        row = stats[o * n_s + j, 3:4]
        seat = lax.broadcasted_iota(jnp.int32, row.shape, 1)
        which = [
            jnp.sum(jnp.where(seat == i * cap + k, row, 0.0), axis=1, keepdims=True) for k in range(cap)
        ]
        for b in range(per_owner):
            acc = jnp.zeros((tokens, blk), f32) if first else mass[:, b * blk:(b + 1) * blk]
            for k in range(cap):
                part = ref[o, :, k * blk:(k + 1) * blk].astype(f32)
                acc = acc + jnp.where(which[k] == float(b), part, 0.0)
            mass[:, b * blk:(b + 1) * blk] = acc

    add_mass(packed, i, True)

    def take_mass(q, carry):
        o = spread(q)
        packed_copy(o, o).wait_recv()
        add_mass(landed, o, False)
        return carry

    lax.fori_loop(1, n_t, take_mass, 0)
    block_wait(stats, n - n_t, st_recv.at[1])
    st = stats[...]
    largest = jnp.max(st, axis=0)[0:1]
    scale = jnp.exp(st[:, 0:1, :] - largest[None])
    line = lax.broadcasted_iota(jnp.int32, st.shape, 1)
    sums = jnp.sum(jnp.where(line == 1, st * scale, st), axis=0)
    total, mass_sum = sums[1:2], sums[2:3]
    rows8 = lax.broadcasted_iota(jnp.int32, (128, tokens), 0)
    back = jnp.where(rows8 == 0, largest, jnp.where(rows8 == 1, loss_scale / total, loss_scale / mass_sum)).T
    factor = jnp.exp(tops[:, 0:1] - back[:, 0:1]) * back[:, 1:2]
    g = shifted[...] * factor - mass[...] * back[:, 2:3]
    grads[0:tokens, :] = g.astype(bf16)
    lg_copy = pltpu.make_async_remote_copy(
        src_ref=grads.at[pl.ds(0, tokens)], dst_ref=grads.at[pl.ds(tokens, tokens)],
        send_sem=pair_sem.at[2], recv_sem=pair_sem.at[3],
        device_id={"dp": other}, device_id_type=MESH)
    lg_copy.start()
    grad_t[...] = g.T.astype(bf16)
    direct = rows % 16 == 0
    if not direct:
        tile = 2 * blk

        def gh_step(k, carry):
            at = pl.multiple_of(k * tile, tile)
            gh_t[pl.ds(at, tile), :] = jnp.dot(weight[pl.ds(at, tile), :], grad_t[...], preferred_element_type=f32)
            return carry

        lax.fori_loop(0, width // tile, gh_step, 0)

    def chunk(ii, jj, begin=0, end=rows):
        start = (ii * n_s + jj) * rows + begin
        if not direct:
            return gh_t[pl.ds(pl.multiple_of(start, 8), end - begin), :]
        return jnp.dot(
            weight[pl.ds(pl.multiple_of(start, 16), end - begin), :], grad_t[...], preferred_element_type=f32)

    hi, lo = i // n_lo, lax.rem(i, n_lo)
    early = in_pair.shape[1]
    rest = rows - early

    def place_of(k):
        q, r = k // n_hi, k % n_hi
        return lax.rem(hi + r, n_hi) * n_lo + lax.rem(lo + q, n_lo)

    def order(p):
        if p == n_s - 1:
            return j
        if p == n_s - 2:
            return j + 1 - 2 * lax.rem(j, 2)
        pairs, jp, pp, member = n_s // 2, j // 2, p // 2, p % 2
        above = pairs - 1 - jp
        low = 2 * jnp.where(pp < above, pairs - 1 - pp, pp - above) + 1 - member
        high = 2 * jnp.where(pp < jp, pp, pairs - 1 - (pp - jp)) + member
        return jnp.where(2 * jp < pairs, low, high)

    mate = order(n_s - 2)

    def slot_of(jj):
        return lax.rem(j // 2 - jj // 2 + n_s // 2, n_s // 2) * 2 - 2 + lax.rem(j, 2)

    def whole_wait(ref, sem):
        pltpu.make_async_copy(ref, ref, sem).wait()

    counts = [0, 0, 0]

    def ship(kind, value, dst, recv, where):
        src = (out, out_pair, out_mate)[kind].at[counts[kind]]
        counts[kind] += 1
        src[...] = value.astype(bf16)
        pltpu.make_async_remote_copy(
            src_ref=src, dst_ref=dst, send_sem=rs_send.at[kind], recv_sem=recv,
            device_id=where, device_id_type=MESH).start()

    def send_dots(p):
        for k in reversed(range(1, n_t)):
            ii = place_of(k)
            if p == n_s - 2:
                ship(2, chunk(ii, mate, early), fin_mate.at[k - 1], fin_sem.at[p], {"tvoc": ii})
            else:
                ship(0, chunk(ii, order(p)), fin.at[p, k - 1], fin_sem.at[p], {"tvoc": ii})

    def pair_dots():
        for k in reversed(range(n_t)):
            ship(1, chunk(place_of(k), mate, 0, early), in_pair.at[k], pair_recv, {"svoc": mate})

    def own_dots():
        for k in reversed(range(n_t)):
            hold[k] = chunk(place_of(k), j)

    def own_send():
        whole_wait(in_pair, pair_recv)
        for k in reversed(range(n_t)):
            hold[k, 0:early] = hold[k, 0:early] + in_pair[k].astype(f32)
            if k:
                ship(0, hold[k], fin.at[n_s - 1, k - 1], fin_sem.at[n_s - 1], {"tvoc": place_of(k)})

    def gather(p):
        if p == n_s - 2:
            acc, terms = own_mate[...], fin_mate
        else:
            acc, terms = own[p] if p < n_s - 1 else hold[0], fin.at[p]
        if n_t > 1:
            whole_wait(terms, fin_sem.at[p])
        for k in range(n_t - 1):
            acc = acc + terms[k].astype(f32)
        return acc

    def finish(p):
        jj = order(p)
        if p == n_s - 2:
            ship(2, gather(p), in_mate, mate_recv, {"svoc": jj})
        else:
            ship(0, gather(p), in_z.at[slot_of(jj)], z_recv, {"svoc": jj})

    tall = 2 * blk
    tiles = half // tall
    done = [0]

    def gw_step(k, carry):
        at = pl.multiple_of(k * tall, tall)
        gw_ref[pl.ds(at, tall), :] = jnp.dot(
            hid_t[pl.ds(at, tall), :], grads[...], preferred_element_type=f32).astype(bf16)
        return carry

    def fill(count):
        until = min(tiles, done[0] + count)
        lax.fori_loop(done[0], until, gw_step, 0)
        done[0] = until

    def spread_late():
        tm = mass[...]
        positive = tm > 0
        stats2[me] = as_rows((
            jnp.sum(jnp.where(positive, tm * jnp.log(jnp.where(positive, tm, 1.0)), 0.0), axis=1, keepdims=True),
            jnp.sum(tm * logits[...], axis=1, keepdims=True)), 2)
        to_all(stats2, st_send.at[1], st_recv.at[2], st_recv.at[2])

    turns = [*range(min(1, n_s - 2)), n_s - 2, *range(1, n_s - 2)]
    for p in turns:
        if p == n_s - 2:
            pair_dots()
        send_dots(p)
    for p in range(n_s - 2):
        own[p] = chunk(i, order(p))
    own_mate[...] = chunk(i, mate, early)
    own_dots()
    spread_late()
    lg_copy.wait_recv()
    fill(tiles)
    own_send()
    for p in turns:
        finish(p)
    block_wait(stats2, n - 1, st_recv.at[2])
    late = jnp.sum(stats2[...], axis=0)
    entropy, cross = late[0:1], late[1:2]
    div_ref[...] = entropy / mass_sum - jnp.log(mass_sum) - cross / mass_sum + largest + jnp.log(total)
    acc = gather(n_s - 1)
    if n_s > 2:
        whole_wait(in_z, z_recv)
    for k in range(n_s - 2):
        acc = acc + in_z[k].astype(f32)
    gh_ref[0:early] = acc[0:early]
    whole_wait(in_mate, mate_recv)
    gh_ref[early:] = acc[early:] + in_mate[...].astype(f32)
    hidden_copy().wait_send()
    lg_copy.wait_send()
    block_wait(packed, n_t - 1, pk_send)
    block_wait(stats, n - 1, st_send.at[0])
    block_wait(stats2, n - 1, st_send.at[1])
    for kind, ref in enumerate((out, out_pair, out_mate)):
        block_wait(ref, counts[kind], rs_send.at[kind])


def flush(div, gw, gh, div_out, gw_out, gh_out, sem):
    copies = [
        pltpu.make_async_copy(src, dst, sem.at[k])
        for k, (src, dst) in enumerate(((gw, gw_out), (gh, gh_out), (div, div_out)))
    ]
    for copy in copies:
        copy.start()
    for copy in copies:
        copy.wait()


def local(n_t, n_s, teacher_probs, block_values, block_index, block_count, hidden, student_weight):
    tokens, width = hidden.shape
    slots, blk = block_values.shape[2], block_values.shape[3]
    shard = student_weight.shape[1]
    half, rows, n = width // 2, width // (n_t * n_s), n_t * n_s
    n_hi, n_lo = split(n_t)
    direct = rows % 16 == 0
    lanes = -(-(n_t * (shard // blk)) // 128) * 128
    vmem = pl.BlockSpec(memory_space=pltpu.VMEM)
    hbm = pl.BlockSpec(memory_space=pltpu.HBM)
    DMA = pltpu.SemaphoreType.DMA
    parcel = (n_t, tokens, cap * blk)
    V = pltpu.VMEM
    early = -(-(rows // 2) // 16) * 16
    rest = rows - early
    exchange = [
        V((n_s - 1, rows, tokens), f32),
        V((rest, tokens), f32),
        V((n_t, rows, tokens), f32),
        V((n_s * n_t, rows, tokens), bf16),
        V((n_t, early, tokens), bf16),
        V((n_t, rest, tokens), bf16),
        V((n_s, n_t - 1, rows, tokens), bf16),
        V((n_t - 1, rest, tokens), bf16),
        V((max(n_s - 2, 1), rows, tokens), bf16),
        V((n_t, early, tokens), bf16),
        V((rest, tokens), bf16),
    ]
    parts = 3 if width % (3 * 128) == 0 else 1
    div, gw, gh = pl.pallas_call(
        functools.partial(kernel, n_t, n_s, blk),
        out_shape=(
            jax.ShapeDtypeStruct((1, tokens), f32),
            jax.ShapeDtypeStruct((half, shard), bf16),
            jax.ShapeDtypeStruct((rows, tokens), f32),
        ),
        in_specs=[hbm] * 6,
        out_specs=(vmem, vmem, vmem),
        scratch_shapes=[
            pltpu.SMEM((1, 1, 2, slots), jnp.int32),
            pltpu.SMEM((1, 1), jnp.int32),
            V((teacher_probs.shape[1] // blk, tokens, blk), bf16),
            V(block_values.shape[2:], bf16),
            V(hidden.shape, bf16),
            V(student_weight.shape, bf16),
            V((tokens, half), bf16),
            V((half, 2 * tokens), bf16),
            V((slots + 1, tokens, blk), f32),
            V((slots, lanes), f32),
            V((1, tokens), f32),
            V((2, lanes), jnp.int32),
            pltpu.SMEM((2, lanes), jnp.int32),
            V(parcel, bf16),
            V(parcel, bf16),
            V((tokens, shard), f32),
            V((tokens, shard), f32),
            V((tokens, shard), f32),
            V((tokens, 128), f32),
            V((n, 4, tokens), f32),
            V((n, 2, tokens), f32),
            V((2 * tokens, shard), bf16),
            V((shard, tokens), bf16),
            V((8, 128) if direct else (width, tokens), f32),
            *exchange,
            DMA((6,)), DMA((parts,)), DMA((4,)), DMA, DMA((n_t,)), DMA((2,)), DMA((3,)),
            DMA((3,)), DMA((n_s,)), DMA, DMA, DMA,
        ],
        compiler_params=pltpu.CompilerParams(
            collective_id=0, has_side_effects=True, vmem_limit_bytes=32 * 1024 * 1024),
    )(
        pltpu.with_memory_space_constraint(jnp.swapaxes(block_index, 2, 3), pltpu.HBM), block_count,
        *(pltpu.with_memory_space_constraint(x, pltpu.HBM) for x in (teacher_probs, block_values, hidden, student_weight)))
    div, gw, gh = pl.pallas_call(
        flush,
        out_shape=tuple(jax.ShapeDtypeStruct(x.shape, x.dtype) for x in (div, gw, gh)),
        in_specs=[vmem] * 3,
        out_specs=(hbm,) * 3,
        scratch_shapes=[DMA((3,))],
        compiler_params=pltpu.CompilerParams(vmem_limit_bytes=2**20),
    )(div, gw, gh)
    return div.reshape(tokens), gw, gh.T


def solution(mesh):
    return jax.shard_map(
        functools.partial(local, mesh.shape["tvoc"], mesh.shape["svoc"]),
        mesh=mesh,
        in_specs=(
            P("dp", "tvoc"),
            P("tvoc", "svoc", None, None, None),
            P("tvoc", "svoc", None, None),
            P("tvoc", "svoc"),
            P("dp", None),
            P(None, ("tvoc", "svoc")),
        ),
        out_specs=(P("dp"), P("dp", ("tvoc", "svoc")), P("dp", ("tvoc", "svoc"))),
        check_vma=False,
    )
```

```python
import functools

import jax
import jax.numpy as jnp
from jax import lax
from jax.experimental import pallas as pl
from jax.experimental.pallas import tpu as pltpu
from jax.sharding import PartitionSpec as P

loss_scale = 128.0
cap = 2
MESH = pl.DeviceIdType.MESH
f32, bf16 = jnp.float32, jnp.bfloat16


def split(n_t):
    n_lo = max(k for k in range(1, n_t + 1) if n_t % k == 0 and k * k <= n_t)
    return n_t // n_lo, n_lo


def kernel(
    n_t, n_s, blk,
    idx_hbm, cnt_hbm, teacher_hbm, values_hbm, hidden_hbm, weight_hbm,
    div_ref, gw_ref, gh_ref,
    idx_s, cnt_s, teacher, values, hidden, weight, peer_hidden, hid_t, mapped, keeps, tags, plan, plan_s,
    packed, landed, mass, logits, shifted, tops, stats, stats2, grads, grad_t, gh_t,
    own, own_mate, hold, out, out_pair, out_mate, fin, fin_mate, in_z, in_pair, in_mate,
    load_sem, weight_sem, pair_sem, pk_send, pk_recv, st_send, st_recv, rs_send, fin_sem, z_recv, pair_recv, mate_recv,
):
    d, i, j = lax.axis_index("dp"), lax.axis_index("tvoc"), lax.axis_index("svoc")
    n_d = 2
    n = n_t * n_s
    n_hi, n_lo = split(n_t)
    me = i * n_s + j
    other = n_d - 1 - d
    tokens, width = hidden.shape
    shard = weight.shape[1]
    per_owner = shard // blk
    half = width // n_d
    rows = width // n
    slots = values.shape[0]

    barrier = pltpu.get_barrier_semaphore()

    def greet(q, carry):
        r = lax.rem(me + q, n)
        pl.semaphore_signal(
            barrier, inc=1, device_id={"tvoc": r // n_s, "svoc": lax.rem(r, n_s)}, device_id_type=MESH)
        return carry

    loads = [
        pltpu.make_async_copy(src, dst, load_sem.at[k])
        for k, (src, dst) in enumerate((
            (idx_hbm, idx_s), (cnt_hbm, cnt_s), (values_hbm.at[0, 0], values), (hidden_hbm, hidden)))
    ]
    parts = weight_sem.shape[0]
    depth = width // parts
    weight_loads = [
        pltpu.make_async_copy(
            weight_hbm.at[pl.ds(k * depth, depth)], weight.at[pl.ds(k * depth, depth)], weight_sem.at[k])
        for k in range(parts)
    ]
    blocks = teacher.shape[0]

    def block_start(b, carry):
        pltpu.make_async_copy(
            teacher_hbm.at[:, pl.ds(pl.multiple_of(b * blk, blk), blk)], teacher.at[b], load_sem.at[4]).start()
        return carry

    loads[2].start()
    loads[0].start()
    loads[1].start()
    loads[3].start()
    lax.fori_loop(1, n, greet, 0)
    pl.semaphore_signal(barrier, inc=1, device_id={"dp": other}, device_id_type=MESH)
    lax.fori_loop(0, blocks, block_start, 0)
    for copy in weight_loads:
        copy.start()
    loads[0].wait()
    loads[1].wait()
    lanes = keeps.shape[1]
    lane = lax.broadcasted_iota(jnp.int32, (slots, lanes), 1)
    slot = lax.broadcasted_iota(jnp.int32, (slots, lanes), 0)
    column = jnp.zeros((slots, lanes), jnp.int32)
    for s in range(slots):
        column = jnp.where(slot == s, idx_s[0, 0, 1, s], column)
    live = slot < cnt_s[0, 0]
    hot = (column == lane) & live
    present = jnp.max(jnp.where(hot, 1.0, 0.0), axis=0, keepdims=True)
    r_iota = lax.broadcasted_iota(jnp.int32, (lanes, lanes), 0).astype(f32)
    c_iota = lax.broadcasted_iota(jnp.int32, (lanes, lanes), 1).astype(f32)
    r_own = jnp.floor((r_iota + 0.5) / per_owner)
    c_own = jnp.floor((c_iota + 0.5) / per_owner)
    below = jnp.where((r_own == c_own) & (r_iota < c_iota), 1.0, 0.0)
    rank = jnp.dot(jnp.broadcast_to(present, (8, lanes)), below, preferred_element_type=f32)[0:1]
    place = cap * c_own[0:1] + rank
    n_tags = n_t * cap
    t_iota = lax.broadcasted_iota(jnp.int32, (n_tags, lanes), 0).astype(f32)
    within = c_iota[0:1] - per_owner * c_own[0:1]
    named = (present > 0.0) & (place == t_iota)
    tag_diag = lax.broadcasted_iota(jnp.int32, (n_tags, lanes), 0) == lax.broadcasted_iota(jnp.int32, (n_tags, lanes), 1)

    def along(col):
        return jnp.sum(jnp.where(tag_diag, jnp.broadcast_to(col, (n_tags, lanes)), 0.0), axis=0, keepdims=True)

    tags[...] = along(jnp.sum(jnp.where(named, within + 1.0, 0.0), axis=1, keepdims=True) - 1.0)[:, 0:tokens]
    upto = jnp.sum(jnp.where(live & (column <= lane), 1.0, 0.0), axis=0, keepdims=True)
    last = jnp.sum(jnp.where(named, upto, 0.0), axis=1, keepdims=True)
    last = jnp.where(last > 0.0, last - 1.0, float(slots))
    slot_f, lane_f = slot.astype(f32), lane.astype(f32)
    diag = slot == lane
    key = jnp.where(live, column * slots, lanes * slots).astype(f32) + slot_f
    key_row = jnp.sum(jnp.where(diag, key, 0.0), axis=0, keepdims=True)
    key_row = jnp.where(lane_f[0:1] < slots, key_row, 2.0 * lanes * slots)
    spot_of = jnp.sum(jnp.where(key_row < key, 1.0, 0.0), axis=1, keepdims=True)
    here = spot_of == lane_f
    plan[0:1] = jnp.sum(jnp.where(here, slot_f, 0.0), axis=0, keepdims=True).astype(jnp.int32)
    plan[1:2] = along(last).astype(jnp.int32)
    plan_copy = pltpu.make_async_copy(plan, plan_s, load_sem.at[5])
    plan_copy.start()
    sorted_row = jnp.sum(jnp.where(here, column.astype(f32), 0.0), axis=0, keepdims=True)
    same = jnp.where(sorted_row == pltpu.roll(sorted_row, 1, 1), 1.0, 0.0)
    keeps[...] = jnp.broadcast_to(jnp.sum(jnp.where(diag, same, 0.0), axis=1, keepdims=True), (slots, lanes))
    mapped[slots] = jnp.zeros((tokens, blk), f32)
    plan_copy.wait()
    loads[2].wait()
    pltpu.make_async_copy(teacher, teacher, load_sem.at[4]).wait()
    run = None
    for k in range(slots):
        s = jnp.clip(plan_s[0, k], 0, slots - 1)
        term = jnp.dot(teacher[idx_s[0, 0, 0, s]], values[s], preferred_element_type=f32)
        run = term if k == 0 else term + keeps[k:k + 1, 0:blk] * run
        mapped[k] = run
    def pack(o, weighed):
        for k in range(cap):
            rounded = mapped[jnp.clip(plan_s[1, o * cap + k], 0, slots)].astype(bf16)
            packed[o, :, k * blk:(k + 1) * blk] = rounded
            weighed = weighed + rounded.astype(f32)
        return weighed

    weighed = lax.fori_loop(0, n_t, pack, jnp.zeros((tokens, blk), f32))
    mass_part = jnp.sum(weighed, axis=1, keepdims=True)
    spot = lax.broadcasted_iota(jnp.int32, (tokens, 128), 1)

    def as_rows(columns, height):
        wide = jnp.zeros((tokens, 128), f32)
        for k, part in enumerate(columns):
            wide = jnp.where(spot == k, part, wide)
        return wide.T[0:height]

    def softmax():
        loads[3].wait()
        for k in range(parts):
            weight_loads[k].wait()
            part = jnp.dot(
                hidden[:, k * depth:(k + 1) * depth], weight[k * depth:(k + 1) * depth, :], preferred_element_type=f32)
            logits[...] = part if k == 0 else logits[...] + part
        lg = logits[...]
        top = jnp.max(lg, axis=1, keepdims=True)
        e = jnp.exp(lg - top)
        shifted[...] = e
        tops[...] = jnp.broadcast_to(top, tops.shape)
        stats[me, 0:3] = as_rows((top, jnp.sum(e, axis=1, keepdims=True), mass_part), 3)
        stats[me, 3:4] = tags[...]

    pl.when(j == 0)(softmax)
    pl.semaphore_wait(barrier, n)
    def spread(k):
        return lax.rem(i // n_lo + lax.rem(k, n_hi), n_hi) * n_lo + lax.rem(i + k // n_hi, n_lo)

    def packed_copy(o, src):
        return pltpu.make_async_remote_copy(
            src_ref=packed.at[o], dst_ref=landed.at[src],
            send_sem=pk_send, recv_sem=pk_recv.at[src],
            device_id={"tvoc": o}, device_id_type=MESH)

    def to_all(ref, send, recv_near, recv_far):
        def start(ii, jj, recv):
            pltpu.make_async_remote_copy(
                src_ref=ref.at[me], dst_ref=ref.at[me], send_sem=send, recv_sem=recv,
                device_id={"tvoc": ii, "svoc": jj}, device_id_type=MESH).start()

        def far(p, carry):
            jj = lax.rem(j + p, n_s)

            def inner(q, c):
                start(lax.rem(i + q, n_t), jj, recv_far)
                return c

            return lax.fori_loop(0, n_t, inner, carry)

        def near(q, carry):
            start(lax.rem(i + q, n_t), j, recv_near)
            return carry

        lax.fori_loop(1, n_s, far, 0)
        lax.fori_loop(1, n_t, near, 0)

    near = [k for k in range(1, n_t) if k % n_hi == 0 or k < n_hi]
    away = [k for k in range(1, n_t) if k not in near]

    def deliver(places):
        for k in places:
            packed_copy(spread(k), i).start()

    def spread_early():
        to_all(stats, st_send.at[0], st_recv.at[0], st_recv.at[1])

    deliver(near)
    pl.when(j != 0)(softmax)
    spread_early()
    deliver(away)
    def hidden_copy():
        start = pl.multiple_of(other * half, blk)
        return pltpu.make_async_remote_copy(
            src_ref=hidden.at[:, pl.ds(start, half)], dst_ref=peer_hidden,
            send_sem=pair_sem.at[0], recv_sem=pair_sem.at[1],
            device_id={"dp": other}, device_id_type=MESH)

    hidden_copy().start()
    own_at = d * half

    def turn_own(k, carry):
        at = pl.multiple_of(k * blk, blk)
        tile = hidden[:, pl.ds(pl.multiple_of(own_at + at, blk), blk)].astype(f32)
        hid_t[pl.ds(at, blk), 0:tokens] = tile.T.astype(bf16)
        return carry

    lax.fori_loop(0, half // blk, turn_own, 0)
    hidden_copy().wait_recv()

    def turn_peer(k, carry):
        at = pl.multiple_of(k * blk, blk)
        hid_t[pl.ds(at, blk), tokens:2 * tokens] = peer_hidden[:, pl.ds(at, blk)].astype(f32).T.astype(bf16)
        return carry

    lax.fori_loop(0, half // blk, turn_peer, 0)
    def block_wait(ref, count, sem):
        pltpu.make_async_copy(ref.at[pl.ds(0, count)], ref.at[pl.ds(0, count)], sem).wait()

    block_wait(stats, n_t - 1, st_recv.at[0])
    def add_mass(ref, o, first):
        row = stats[o * n_s + j, 3:4]
        seat = lax.broadcasted_iota(jnp.int32, row.shape, 1)
        which = [
            jnp.sum(jnp.where(seat == i * cap + k, row, 0.0), axis=1, keepdims=True) for k in range(cap)
        ]
        for b in range(per_owner):
            acc = jnp.zeros((tokens, blk), f32) if first else mass[:, b * blk:(b + 1) * blk]
            for k in range(cap):
                part = ref[o, :, k * blk:(k + 1) * blk].astype(f32)
                acc = acc + jnp.where(which[k] == float(b), part, 0.0)
            mass[:, b * blk:(b + 1) * blk] = acc

    add_mass(packed, i, True)

    def take_mass(q, carry):
        o = spread(q)
        packed_copy(o, o).wait_recv()
        add_mass(landed, o, False)
        return carry

    lax.fori_loop(1, n_t, take_mass, 0)
    block_wait(stats, n - n_t, st_recv.at[1])
    st = stats[...]
    largest = jnp.max(st, axis=0)[0:1]
    scale = jnp.exp(st[:, 0:1, :] - largest[None])
    line = lax.broadcasted_iota(jnp.int32, st.shape, 1)
    sums = jnp.sum(jnp.where(line == 1, st * scale, st), axis=0)
    total, mass_sum = sums[1:2], sums[2:3]
    rows8 = lax.broadcasted_iota(jnp.int32, (128, tokens), 0)
    back = jnp.where(rows8 == 0, largest, jnp.where(rows8 == 1, loss_scale / total, loss_scale / mass_sum)).T
    factor = jnp.exp(tops[:, 0:1] - back[:, 0:1]) * back[:, 1:2]
    g = shifted[...] * factor - mass[...] * back[:, 2:3]
    grads[0:tokens, :] = g.astype(bf16)
    lg_copy = pltpu.make_async_remote_copy(
        src_ref=grads.at[pl.ds(0, tokens)], dst_ref=grads.at[pl.ds(tokens, tokens)],
        send_sem=pair_sem.at[2], recv_sem=pair_sem.at[3],
        device_id={"dp": other}, device_id_type=MESH)
    lg_copy.start()
    grad_t[...] = g.T.astype(bf16)
    direct = rows % 16 == 0
    if not direct:
        tile = 2 * blk

        def gh_step(k, carry):
            at = pl.multiple_of(k * tile, tile)
            gh_t[pl.ds(at, tile), :] = jnp.dot(weight[pl.ds(at, tile), :], grad_t[...], preferred_element_type=f32)
            return carry

        lax.fori_loop(0, width // tile, gh_step, 0)

    def chunk(ii, jj, begin=0, end=rows):
        start = (ii * n_s + jj) * rows + begin
        if not direct:
            return gh_t[pl.ds(pl.multiple_of(start, 8), end - begin), :]
        return jnp.dot(
            weight[pl.ds(pl.multiple_of(start, 16), end - begin), :], grad_t[...], preferred_element_type=f32)

    hi, lo = i // n_lo, lax.rem(i, n_lo)
    early = in_pair.shape[1]
    rest = rows - early

    def place_of(k):
        q, r = k // n_hi, k % n_hi
        return lax.rem(hi + r, n_hi) * n_lo + lax.rem(lo + q, n_lo)

    def order(p):
        if p == n_s - 1:
            return j
        if p == n_s - 2:
            return j + 1 - 2 * lax.rem(j, 2)
        pairs, jp, pp, member = n_s // 2, j // 2, p // 2, p % 2
        above = pairs - 1 - jp
        low = 2 * jnp.where(pp < above, pairs - 1 - pp, pp - above) + 1 - member
        high = 2 * jnp.where(pp < jp, pp, pairs - 1 - (pp - jp)) + member
        return jnp.where(2 * jp < pairs, low, high)

    mate = order(n_s - 2)

    def slot_of(jj):
        return lax.rem(j // 2 - jj // 2 + n_s // 2, n_s // 2) * 2 - 2 + lax.rem(j, 2)

    def whole_wait(ref, sem):
        pltpu.make_async_copy(ref, ref, sem).wait()

    counts = [0, 0, 0]

    def ship(kind, value, dst, recv, where):
        src = (out, out_pair, out_mate)[kind].at[counts[kind]]
        counts[kind] += 1
        src[...] = value.astype(bf16)
        pltpu.make_async_remote_copy(
            src_ref=src, dst_ref=dst, send_sem=rs_send.at[kind], recv_sem=recv,
            device_id=where, device_id_type=MESH).start()

    def send_dots(p):
        for k in reversed(range(1, n_t)):
            ii = place_of(k)
            if p == n_s - 2:
                ship(2, chunk(ii, mate, early), fin_mate.at[k - 1], fin_sem.at[p], {"tvoc": ii})
            else:
                ship(0, chunk(ii, order(p)), fin.at[p, k - 1], fin_sem.at[p], {"tvoc": ii})

    def pair_dots():
        for k in reversed(range(n_t)):
            ship(1, chunk(place_of(k), mate, 0, early), in_pair.at[k], pair_recv, {"svoc": mate})

    def own_dots():
        for k in reversed(range(n_t)):
            hold[k] = chunk(place_of(k), j)

    def own_send():
        whole_wait(in_pair, pair_recv)
        for k in reversed(range(n_t)):
            hold[k, 0:early] = hold[k, 0:early] + in_pair[k].astype(f32)
            if k:
                ship(0, hold[k], fin.at[n_s - 1, k - 1], fin_sem.at[n_s - 1], {"tvoc": place_of(k)})

    def gather(p):
        if p == n_s - 2:
            acc, terms = own_mate[...], fin_mate
        else:
            acc, terms = own[p] if p < n_s - 1 else hold[0], fin.at[p]
        if n_t > 1:
            whole_wait(terms, fin_sem.at[p])
        for k in range(n_t - 1):
            acc = acc + terms[k].astype(f32)
        return acc

    def finish(p):
        jj = order(p)
        if p == n_s - 2:
            ship(2, gather(p), in_mate, mate_recv, {"svoc": jj})
        else:
            ship(0, gather(p), in_z.at[slot_of(jj)], z_recv, {"svoc": jj})

    tall = 2 * blk
    tiles = half // tall
    done = [0]

    def gw_step(k, carry):
        at = pl.multiple_of(k * tall, tall)
        gw_ref[pl.ds(at, tall), :] = jnp.dot(
            hid_t[pl.ds(at, tall), :], grads[...], preferred_element_type=f32).astype(bf16)
        return carry

    def fill(count):
        until = min(tiles, done[0] + count)
        lax.fori_loop(done[0], until, gw_step, 0)
        done[0] = until

    def spread_late():
        tm = mass[...]
        positive = tm > 0
        stats2[me] = as_rows((
            jnp.sum(jnp.where(positive, tm * jnp.log(jnp.where(positive, tm, 1.0)), 0.0), axis=1, keepdims=True),
            jnp.sum(tm * logits[...], axis=1, keepdims=True)), 2)
        to_all(stats2, st_send.at[1], st_recv.at[2], st_recv.at[2])

    low = j // 2 * 2 < n_s // 2
    others = list(range(n_s - 2))

    def by_half(work):
        kept = list(counts)
        pl.when(low)(functools.partial(work, [n_s - 2, *others]))
        counts[:] = kept
        pl.when(jnp.logical_not(low))(functools.partial(work, [*others, n_s - 2]))

    def send_all(turns):
        for at, p in enumerate(turns):
            send_dots(p)
            if p == 0 or n_s == 2:
                pair_dots()

    def finish_all(turns):
        for p in turns:
            finish(p)

    by_half(send_all)
    for p in range(n_s - 2):
        own[p] = chunk(i, order(p))
    own_mate[...] = chunk(i, mate, early)
    own_dots()
    spread_late()
    lg_copy.wait_recv()
    fill(tiles)
    own_send()
    by_half(finish_all)
    block_wait(stats2, n - 1, st_recv.at[2])
    late = jnp.sum(stats2[...], axis=0)
    entropy, cross = late[0:1], late[1:2]
    div_ref[...] = entropy / mass_sum - jnp.log(mass_sum) - cross / mass_sum + largest + jnp.log(total)
    acc = gather(n_s - 1)
    if n_s > 2:
        whole_wait(in_z, z_recv)
    for k in range(n_s - 2):
        acc = acc + in_z[k].astype(f32)
    gh_ref[0:early] = acc[0:early]
    whole_wait(in_mate, mate_recv)
    gh_ref[early:] = acc[early:] + in_mate[...].astype(f32)
    hidden_copy().wait_send()
    lg_copy.wait_send()
    block_wait(packed, n_t - 1, pk_send)
    block_wait(stats, n - 1, st_send.at[0])
    block_wait(stats2, n - 1, st_send.at[1])
    for kind, ref in enumerate((out, out_pair, out_mate)):
        block_wait(ref, counts[kind], rs_send.at[kind])


def flush(div, gw, gh, div_out, gw_out, gh_out, sem):
    copies = [
        pltpu.make_async_copy(src, dst, sem.at[k])
        for k, (src, dst) in enumerate(((gw, gw_out), (gh, gh_out), (div, div_out)))
    ]
    for copy in copies:
        copy.start()
    for copy in copies:
        copy.wait()


def local(n_t, n_s, teacher_probs, block_values, block_index, block_count, hidden, student_weight):
    tokens, width = hidden.shape
    slots, blk = block_values.shape[2], block_values.shape[3]
    shard = student_weight.shape[1]
    half, rows, n = width // 2, width // (n_t * n_s), n_t * n_s
    n_hi, n_lo = split(n_t)
    direct = rows % 16 == 0
    lanes = -(-(n_t * (shard // blk)) // 128) * 128
    vmem = pl.BlockSpec(memory_space=pltpu.VMEM)
    hbm = pl.BlockSpec(memory_space=pltpu.HBM)
    DMA = pltpu.SemaphoreType.DMA
    parcel = (n_t, tokens, cap * blk)
    V = pltpu.VMEM
    early = -(-(rows // 2) // 16) * 16
    rest = rows - early
    exchange = [
        V((n_s - 1, rows, tokens), f32),
        V((rest, tokens), f32),
        V((n_t, rows, tokens), f32),
        V((n_s * n_t, rows, tokens), bf16),
        V((n_t, early, tokens), bf16),
        V((n_t, rest, tokens), bf16),
        V((n_s, n_t - 1, rows, tokens), bf16),
        V((n_t - 1, rest, tokens), bf16),
        V((max(n_s - 2, 1), rows, tokens), bf16),
        V((n_t, early, tokens), bf16),
        V((rest, tokens), bf16),
    ]
    parts = 3 if width % (3 * 128) == 0 else 1
    div, gw, gh = pl.pallas_call(
        functools.partial(kernel, n_t, n_s, blk),
        out_shape=(
            jax.ShapeDtypeStruct((1, tokens), f32),
            jax.ShapeDtypeStruct((half, shard), bf16),
            jax.ShapeDtypeStruct((rows, tokens), f32),
        ),
        in_specs=[hbm] * 6,
        out_specs=(vmem, vmem, vmem),
        scratch_shapes=[
            pltpu.SMEM((1, 1, 2, slots), jnp.int32),
            pltpu.SMEM((1, 1), jnp.int32),
            V((teacher_probs.shape[1] // blk, tokens, blk), bf16),
            V(block_values.shape[2:], bf16),
            V(hidden.shape, bf16),
            V(student_weight.shape, bf16),
            V((tokens, half), bf16),
            V((half, 2 * tokens), bf16),
            V((slots + 1, tokens, blk), f32),
            V((slots, lanes), f32),
            V((1, tokens), f32),
            V((2, lanes), jnp.int32),
            pltpu.SMEM((2, lanes), jnp.int32),
            V(parcel, bf16),
            V(parcel, bf16),
            V((tokens, shard), f32),
            V((tokens, shard), f32),
            V((tokens, shard), f32),
            V((tokens, 128), f32),
            V((n, 4, tokens), f32),
            V((n, 2, tokens), f32),
            V((2 * tokens, shard), bf16),
            V((shard, tokens), bf16),
            V((8, 128) if direct else (width, tokens), f32),
            *exchange,
            DMA((6,)), DMA((parts,)), DMA((4,)), DMA, DMA((n_t,)), DMA((2,)), DMA((3,)),
            DMA((3,)), DMA((n_s,)), DMA, DMA, DMA,
        ],
        compiler_params=pltpu.CompilerParams(
            collective_id=0, has_side_effects=True, vmem_limit_bytes=32 * 1024 * 1024),
    )(
        pltpu.with_memory_space_constraint(jnp.swapaxes(block_index, 2, 3), pltpu.HBM), block_count,
        *(pltpu.with_memory_space_constraint(x, pltpu.HBM) for x in (teacher_probs, block_values, hidden, student_weight)))
    div, gw, gh = pl.pallas_call(
        flush,
        out_shape=tuple(jax.ShapeDtypeStruct(x.shape, x.dtype) for x in (div, gw, gh)),
        in_specs=[vmem] * 3,
        out_specs=(hbm,) * 3,
        scratch_shapes=[DMA((3,))],
        compiler_params=pltpu.CompilerParams(vmem_limit_bytes=2**20),
    )(div, gw, gh)
    return div.reshape(tokens), gw, gh.T


def solution(mesh):
    return jax.shard_map(
        functools.partial(local, mesh.shape["tvoc"], mesh.shape["svoc"]),
        mesh=mesh,
        in_specs=(
            P("dp", "tvoc"),
            P("tvoc", "svoc", None, None, None),
            P("tvoc", "svoc", None, None),
            P("tvoc", "svoc"),
            P("dp", None),
            P(None, ("tvoc", "svoc")),
        ),
        out_specs=(P("dp"), P("dp", ("tvoc", "svoc")), P("dp", ("tvoc", "svoc"))),
        check_vma=False,
    )
```

```python
import functools

import jax
import jax.numpy as jnp
from jax import lax
from jax.experimental import pallas as pl
from jax.experimental.pallas import tpu as pltpu
from jax.sharding import PartitionSpec as P

loss_scale = 128.0
cap = 2
MESH = pl.DeviceIdType.MESH
f32, bf16 = jnp.float32, jnp.bfloat16


def split(n_t):
    n_lo = max(k for k in range(1, n_t + 1) if n_t % k == 0 and k * k <= n_t)
    return n_t // n_lo, n_lo


def kernel(
    n_t, n_s, blk,
    idx_hbm, cnt_hbm, teacher_hbm, values_hbm, hidden_hbm, weight_hbm,
    div_ref, gw_ref, gh_ref,
    idx_s, cnt_s, teacher, values, hidden, weight, peer_hidden, hid_t, mapped, keeps, tags, plan, plan_s,
    packed, landed, mass, logits, shifted, tops, stats, stats2, grads, grad_t, gh_t,
    own, own_mate, hold, out, out_pair, out_mate, fin, fin_mate, in_z, in_pair, in_mate,
    load_sem, weight_sem, pair_sem, pk_send, pk_recv, st_send, st_recv, rs_send, fin_sem, z_recv, pair_recv, mate_recv,
):
    d, i, j = lax.axis_index("dp"), lax.axis_index("tvoc"), lax.axis_index("svoc")
    n_d = 2
    n = n_t * n_s
    n_hi, n_lo = split(n_t)
    me = i * n_s + j
    other = n_d - 1 - d
    tokens, width = hidden.shape
    shard = weight.shape[1]
    per_owner = shard // blk
    half = width // n_d
    rows = width // n
    slots = values.shape[0]

    barrier = pltpu.get_barrier_semaphore()

    def greet(q, carry):
        r = lax.rem(me + q, n)
        pl.semaphore_signal(
            barrier, inc=1, device_id={"tvoc": r // n_s, "svoc": lax.rem(r, n_s)}, device_id_type=MESH)
        return carry

    loads = [
        pltpu.make_async_copy(src, dst, load_sem.at[k])
        for k, (src, dst) in enumerate((
            (idx_hbm, idx_s), (cnt_hbm, cnt_s), (values_hbm.at[0, 0], values), (hidden_hbm, hidden)))
    ]
    parts = weight_sem.shape[0]
    depth = width // parts
    weight_loads = [
        pltpu.make_async_copy(
            weight_hbm.at[pl.ds(k * depth, depth)], weight.at[pl.ds(k * depth, depth)], weight_sem.at[k])
        for k in range(parts)
    ]
    blocks = teacher.shape[0]

    def block_start(b, carry):
        pltpu.make_async_copy(
            teacher_hbm.at[:, pl.ds(pl.multiple_of(b * blk, blk), blk)], teacher.at[b], load_sem.at[4]).start()
        return carry

    loads[2].start()
    loads[0].start()
    loads[1].start()
    loads[3].start()
    lax.fori_loop(1, n, greet, 0)
    pl.semaphore_signal(barrier, inc=1, device_id={"dp": other}, device_id_type=MESH)
    lax.fori_loop(0, blocks, block_start, 0)
    for copy in weight_loads:
        copy.start()
    loads[0].wait()
    loads[1].wait()
    lanes = keeps.shape[1]
    lane = lax.broadcasted_iota(jnp.int32, (slots, lanes), 1)
    slot = lax.broadcasted_iota(jnp.int32, (slots, lanes), 0)
    column = jnp.zeros((slots, lanes), jnp.int32)
    for s in range(slots):
        column = jnp.where(slot == s, idx_s[0, 0, 1, s], column)
    live = slot < cnt_s[0, 0]
    hot = (column == lane) & live
    present = jnp.max(jnp.where(hot, 1.0, 0.0), axis=0, keepdims=True)
    r_iota = lax.broadcasted_iota(jnp.int32, (lanes, lanes), 0).astype(f32)
    c_iota = lax.broadcasted_iota(jnp.int32, (lanes, lanes), 1).astype(f32)
    r_own = jnp.floor((r_iota + 0.5) / per_owner)
    c_own = jnp.floor((c_iota + 0.5) / per_owner)
    below = jnp.where((r_own == c_own) & (r_iota < c_iota), 1.0, 0.0)
    rank = jnp.dot(jnp.broadcast_to(present, (8, lanes)), below, preferred_element_type=f32)[0:1]
    place = cap * c_own[0:1] + rank
    n_tags = n_t * cap
    t_iota = lax.broadcasted_iota(jnp.int32, (n_tags, lanes), 0).astype(f32)
    within = c_iota[0:1] - per_owner * c_own[0:1]
    named = (present > 0.0) & (place == t_iota)
    tag_diag = lax.broadcasted_iota(jnp.int32, (n_tags, lanes), 0) == lax.broadcasted_iota(jnp.int32, (n_tags, lanes), 1)

    def along(col):
        return jnp.sum(jnp.where(tag_diag, jnp.broadcast_to(col, (n_tags, lanes)), 0.0), axis=0, keepdims=True)

    tags[...] = along(jnp.sum(jnp.where(named, within + 1.0, 0.0), axis=1, keepdims=True) - 1.0)[:, 0:tokens]
    upto = jnp.sum(jnp.where(live & (column <= lane), 1.0, 0.0), axis=0, keepdims=True)
    last = jnp.sum(jnp.where(named, upto, 0.0), axis=1, keepdims=True)
    last = jnp.where(last > 0.0, last - 1.0, float(slots))
    slot_f, lane_f = slot.astype(f32), lane.astype(f32)
    diag = slot == lane
    key = jnp.where(live, column * slots, lanes * slots).astype(f32) + slot_f
    key_row = jnp.sum(jnp.where(diag, key, 0.0), axis=0, keepdims=True)
    key_row = jnp.where(lane_f[0:1] < slots, key_row, 2.0 * lanes * slots)
    spot_of = jnp.sum(jnp.where(key_row < key, 1.0, 0.0), axis=1, keepdims=True)
    here = spot_of == lane_f
    plan[0:1] = jnp.sum(jnp.where(here, slot_f, 0.0), axis=0, keepdims=True).astype(jnp.int32)
    plan[1:2] = along(last).astype(jnp.int32)
    plan_copy = pltpu.make_async_copy(plan, plan_s, load_sem.at[5])
    plan_copy.start()
    sorted_row = jnp.sum(jnp.where(here, column.astype(f32), 0.0), axis=0, keepdims=True)
    same = jnp.where(sorted_row == pltpu.roll(sorted_row, 1, 1), 1.0, 0.0)
    keeps[...] = jnp.broadcast_to(jnp.sum(jnp.where(diag, same, 0.0), axis=1, keepdims=True), (slots, lanes))
    mapped[slots] = jnp.zeros((tokens, blk), f32)
    plan_copy.wait()
    loads[2].wait()
    pltpu.make_async_copy(teacher, teacher, load_sem.at[4]).wait()
    run = None
    for k in range(slots):
        s = jnp.clip(plan_s[0, k], 0, slots - 1)
        term = jnp.dot(teacher[idx_s[0, 0, 0, s]], values[s], preferred_element_type=f32)
        run = term if k == 0 else term + keeps[k:k + 1, 0:blk] * run
        mapped[k] = run
    def pack(o, weighed):
        for k in range(cap):
            rounded = mapped[jnp.clip(plan_s[1, o * cap + k], 0, slots)].astype(bf16)
            packed[o, :, k * blk:(k + 1) * blk] = rounded
            weighed = weighed + rounded.astype(f32)
        return weighed

    weighed = lax.fori_loop(0, n_t, pack, jnp.zeros((tokens, blk), f32))
    mass_part = jnp.sum(weighed, axis=1, keepdims=True)
    spot = lax.broadcasted_iota(jnp.int32, (tokens, 128), 1)

    def as_rows(columns, height):
        wide = jnp.zeros((tokens, 128), f32)
        for k, part in enumerate(columns):
            wide = jnp.where(spot == k, part, wide)
        return wide.T[0:height]

    def softmax():
        loads[3].wait()
        for k in range(parts):
            weight_loads[k].wait()
            part = jnp.dot(
                hidden[:, k * depth:(k + 1) * depth], weight[k * depth:(k + 1) * depth, :], preferred_element_type=f32)
            logits[...] = part if k == 0 else logits[...] + part
        lg = logits[...]
        top = jnp.max(lg, axis=1, keepdims=True)
        e = jnp.exp(lg - top)
        shifted[...] = e
        tops[...] = jnp.broadcast_to(top, tops.shape)
        stats[me, 0:3] = as_rows((top, jnp.sum(e, axis=1, keepdims=True), mass_part), 3)
        stats[me, 3:4] = tags[...]

    pl.when(j == 0)(softmax)
    pl.semaphore_wait(barrier, n)
    def spread(k):
        return lax.rem(i // n_lo + lax.rem(k, n_hi), n_hi) * n_lo + lax.rem(i + k // n_hi, n_lo)

    def packed_copy(o, src):
        return pltpu.make_async_remote_copy(
            src_ref=packed.at[o], dst_ref=landed.at[src],
            send_sem=pk_send, recv_sem=pk_recv.at[src],
            device_id={"tvoc": o}, device_id_type=MESH)

    def to_all(ref, send, recv_near, recv_far):
        def start(ii, jj, recv):
            pltpu.make_async_remote_copy(
                src_ref=ref.at[me], dst_ref=ref.at[me], send_sem=send, recv_sem=recv,
                device_id={"tvoc": ii, "svoc": jj}, device_id_type=MESH).start()

        def far(p, carry):
            jj = lax.rem(j + p, n_s)

            def inner(q, c):
                start(lax.rem(i + q, n_t), jj, recv_far)
                return c

            return lax.fori_loop(0, n_t, inner, carry)

        def near(q, carry):
            start(lax.rem(i + q, n_t), j, recv_near)
            return carry

        lax.fori_loop(1, n_s, far, 0)
        lax.fori_loop(1, n_t, near, 0)

    near = [k for k in range(1, n_t) if k % n_hi == 0 or k < n_hi]
    away = [k for k in range(1, n_t) if k not in near]

    def deliver(places):
        for k in places:
            packed_copy(spread(k), i).start()

    def spread_early():
        to_all(stats, st_send.at[0], st_recv.at[0], st_recv.at[1])

    deliver(near)
    pl.when(j != 0)(softmax)
    spread_early()
    deliver(away)
    def hidden_copy():
        start = pl.multiple_of(other * half, blk)
        return pltpu.make_async_remote_copy(
            src_ref=hidden.at[:, pl.ds(start, half)], dst_ref=peer_hidden,
            send_sem=pair_sem.at[0], recv_sem=pair_sem.at[1],
            device_id={"dp": other}, device_id_type=MESH)

    hidden_copy().start()
    own_at = d * half

    def turn_own(k, carry):
        at = pl.multiple_of(k * blk, blk)
        tile = hidden[:, pl.ds(pl.multiple_of(own_at + at, blk), blk)].astype(f32)
        hid_t[pl.ds(at, blk), 0:tokens] = tile.T.astype(bf16)
        return carry

    lax.fori_loop(0, half // blk, turn_own, 0)
    hidden_copy().wait_recv()

    def turn_peer(k, carry):
        at = pl.multiple_of(k * blk, blk)
        hid_t[pl.ds(at, blk), tokens:2 * tokens] = peer_hidden[:, pl.ds(at, blk)].astype(f32).T.astype(bf16)
        return carry

    lax.fori_loop(0, half // blk, turn_peer, 0)
    def block_wait(ref, count, sem):
        pltpu.make_async_copy(ref.at[pl.ds(0, count)], ref.at[pl.ds(0, count)], sem).wait()

    block_wait(stats, n_t - 1, st_recv.at[0])
    def add_mass(ref, o, first):
        row = stats[o * n_s + j, 3:4]
        seat = lax.broadcasted_iota(jnp.int32, row.shape, 1)
        which = [
            jnp.sum(jnp.where(seat == i * cap + k, row, 0.0), axis=1, keepdims=True) for k in range(cap)
        ]
        for b in range(per_owner):
            acc = jnp.zeros((tokens, blk), f32) if first else mass[:, b * blk:(b + 1) * blk]
            for k in range(cap):
                part = ref[o, :, k * blk:(k + 1) * blk].astype(f32)
                acc = acc + jnp.where(which[k] == float(b), part, 0.0)
            mass[:, b * blk:(b + 1) * blk] = acc

    add_mass(packed, i, True)

    def take_mass(q, carry):
        o = spread(q)
        packed_copy(o, o).wait_recv()
        add_mass(landed, o, False)
        return carry

    lax.fori_loop(1, n_t, take_mass, 0)
    block_wait(stats, n - n_t, st_recv.at[1])
    st = stats[...]
    largest = jnp.max(st, axis=0)[0:1]
    scale = jnp.exp(st[:, 0:1, :] - largest[None])
    line = lax.broadcasted_iota(jnp.int32, st.shape, 1)
    sums = jnp.sum(jnp.where(line == 1, st * scale, st), axis=0)
    total, mass_sum = sums[1:2], sums[2:3]
    rows8 = lax.broadcasted_iota(jnp.int32, (128, tokens), 0)
    back = jnp.where(rows8 == 0, largest, jnp.where(rows8 == 1, loss_scale / total, loss_scale / mass_sum)).T
    factor = jnp.exp(tops[:, 0:1] - back[:, 0:1]) * back[:, 1:2]
    g = shifted[...] * factor - mass[...] * back[:, 2:3]
    grads[0:tokens, :] = g.astype(bf16)
    lg_copy = pltpu.make_async_remote_copy(
        src_ref=grads.at[pl.ds(0, tokens)], dst_ref=grads.at[pl.ds(tokens, tokens)],
        send_sem=pair_sem.at[2], recv_sem=pair_sem.at[3],
        device_id={"dp": other}, device_id_type=MESH)
    lg_copy.start()
    grad_t[...] = g.T.astype(bf16)
    direct = rows % 16 == 0
    if not direct:
        tile = 2 * blk

        def gh_step(k, carry):
            at = pl.multiple_of(k * tile, tile)
            gh_t[pl.ds(at, tile), :] = jnp.dot(weight[pl.ds(at, tile), :], grad_t[...], preferred_element_type=f32)
            return carry

        lax.fori_loop(0, width // tile, gh_step, 0)

    def chunk(ii, jj, begin=0, end=rows):
        start = (ii * n_s + jj) * rows + begin
        if not direct:
            return gh_t[pl.ds(pl.multiple_of(start, 8), end - begin), :]
        return jnp.dot(
            weight[pl.ds(pl.multiple_of(start, 16), end - begin), :], grad_t[...], preferred_element_type=f32)

    hi, lo = i // n_lo, lax.rem(i, n_lo)
    early = in_pair.shape[1]
    rest = rows - early

    def place_of(k):
        q, r = k // n_hi, k % n_hi
        return lax.rem(hi + r, n_hi) * n_lo + lax.rem(lo + q, n_lo)

    def order(p):
        if p == n_s - 1:
            return j
        if p == n_s - 2:
            return j + 1 - 2 * lax.rem(j, 2)
        pairs, jp, pp, member = n_s // 2, j // 2, p // 2, p % 2
        above = pairs - 1 - jp
        low = 2 * jnp.where(pp < above, pairs - 1 - pp, pp - above) + 1 - member
        high = 2 * jnp.where(pp < jp, pp, pairs - 1 - (pp - jp)) + member
        return jnp.where(2 * jp < pairs, low, high)

    mate = order(n_s - 2)

    def slot_of(jj):
        return lax.rem(j // 2 - jj // 2 + n_s // 2, n_s // 2) * 2 - 2 + lax.rem(j, 2)

    def whole_wait(ref, sem):
        pltpu.make_async_copy(ref, ref, sem).wait()

    counts = [0, 0, 0]

    def ship(kind, value, dst, recv, where):
        src = (out, out_pair, out_mate)[kind].at[counts[kind]]
        counts[kind] += 1
        src[...] = value.astype(bf16)
        pltpu.make_async_remote_copy(
            src_ref=src, dst_ref=dst, send_sem=rs_send.at[kind], recv_sem=recv,
            device_id=where, device_id_type=MESH).start()

    def send_dots(p):
        for k in reversed(range(1, n_t)):
            ii = place_of(k)
            if p == n_s - 2:
                ship(2, chunk(ii, mate, early), fin_mate.at[k - 1], fin_sem.at[p], {"tvoc": ii})
            else:
                ship(0, chunk(ii, order(p)), fin.at[p, k - 1], fin_sem.at[p], {"tvoc": ii})

    def pair_dots():
        for k in reversed(range(n_t)):
            ship(1, chunk(place_of(k), mate, 0, early), in_pair.at[k], pair_recv, {"svoc": mate})

    def own_dots():
        for k in reversed(range(n_t)):
            hold[k] = chunk(place_of(k), j)

    def own_send():
        whole_wait(in_pair, pair_recv)
        for k in reversed(range(n_t)):
            hold[k, 0:early] = hold[k, 0:early] + in_pair[k].astype(f32)
            if k:
                ship(0, hold[k], fin.at[n_s - 1, k - 1], fin_sem.at[n_s - 1], {"tvoc": place_of(k)})

    def gather(p):
        if p == n_s - 2:
            acc, terms = own_mate[...], fin_mate
        else:
            acc, terms = own[p] if p < n_s - 1 else hold[0], fin.at[p]
        if n_t > 1:
            whole_wait(terms, fin_sem.at[p])
        for k in range(n_t - 1):
            acc = acc + terms[k].astype(f32)
        return acc

    def finish(p):
        jj = order(p)
        if p == n_s - 2:
            ship(2, gather(p), in_mate, mate_recv, {"svoc": jj})
        else:
            ship(0, gather(p), in_z.at[slot_of(jj)], z_recv, {"svoc": jj})

    tall = 2 * blk
    tiles = half // tall
    done = [0]

    def gw_step(k, carry):
        at = pl.multiple_of(k * tall, tall)
        gw_ref[pl.ds(at, tall), :] = jnp.dot(
            hid_t[pl.ds(at, tall), :], grads[...], preferred_element_type=f32).astype(bf16)
        return carry

    def fill(count):
        until = min(tiles, done[0] + count)
        lax.fori_loop(done[0], until, gw_step, 0)
        done[0] = until

    def spread_late():
        tm = mass[...]
        positive = tm > 0
        stats2[me] = as_rows((
            jnp.sum(jnp.where(positive, tm * jnp.log(jnp.where(positive, tm, 1.0)), 0.0), axis=1, keepdims=True),
            jnp.sum(tm * logits[...], axis=1, keepdims=True)), 2)
        to_all(stats2, st_send.at[1], st_recv.at[2], st_recv.at[2])

    low = j // 2 * 2 < n_s // 2
    others = list(range(n_s - 2))

    def by_half(work):
        kept = list(counts)
        pl.when(low)(functools.partial(work, [n_s - 2, *others]))
        counts[:] = kept
        pl.when(jnp.logical_not(low))(functools.partial(work, [*others, n_s - 2]))

    def send_all(turns):
        for at, p in enumerate(turns):
            send_dots(p)
            if p == 0 or n_s == 2:
                pair_dots()

    def finish_all(turns):
        for p in turns:
            finish(p)

    by_half(send_all)
    for p in range(n_s - 2):
        own[p] = chunk(i, order(p))
    own_mate[...] = chunk(i, mate, early)
    own_dots()
    spread_late()
    lg_copy.wait_recv()
    fill(tiles)
    own_send()
    by_half(finish_all)
    block_wait(stats2, n - 1, st_recv.at[2])
    late = jnp.sum(stats2[...], axis=0)
    entropy, cross = late[0:1], late[1:2]
    div_ref[...] = entropy / mass_sum - jnp.log(mass_sum) - cross / mass_sum + largest + jnp.log(total)
    acc = gather(n_s - 1)
    if n_s > 2:
        whole_wait(in_z, z_recv)
    for k in range(n_s - 2):
        acc = acc + in_z[k].astype(f32)
    gh_ref[0:early] = acc[0:early]
    whole_wait(in_mate, mate_recv)
    gh_ref[early:] = acc[early:] + in_mate[...].astype(f32)
    hidden_copy().wait_send()
    lg_copy.wait_send()
    block_wait(packed, n_t - 1, pk_send)
    block_wait(stats, n - 1, st_send.at[0])
    block_wait(stats2, n - 1, st_send.at[1])
    for kind, ref in enumerate((out, out_pair, out_mate)):
        block_wait(ref, counts[kind], rs_send.at[kind])


def flush(div, gw, gh, div_out, gw_out, gh_out, sem):
    copies = [
        pltpu.make_async_copy(src, dst, sem.at[k])
        for k, (src, dst) in enumerate(((gw, gw_out), (gh, gh_out), (div, div_out)))
    ]
    for copy in copies:
        copy.start()
    for copy in copies:
        copy.wait()


def local(n_t, n_s, teacher_probs, block_values, block_index, block_count, hidden, student_weight):
    tokens, width = hidden.shape
    slots, blk = block_values.shape[2], block_values.shape[3]
    shard = student_weight.shape[1]
    half, rows, n = width // 2, width // (n_t * n_s), n_t * n_s
    n_hi, n_lo = split(n_t)
    direct = rows % 16 == 0
    lanes = -(-(n_t * (shard // blk)) // 128) * 128
    vmem = pl.BlockSpec(memory_space=pltpu.VMEM)
    hbm = pl.BlockSpec(memory_space=pltpu.HBM)
    DMA = pltpu.SemaphoreType.DMA
    parcel = (n_t, tokens, cap * blk)
    V = pltpu.VMEM
    early = -(-(rows // 2) // 16) * 16
    rest = rows - early
    exchange = [
        V((n_s - 1, rows, tokens), f32),
        V((rest, tokens), f32),
        V((n_t, rows, tokens), f32),
        V((n_s * n_t, rows, tokens), bf16),
        V((n_t, early, tokens), bf16),
        V((n_t, rest, tokens), bf16),
        V((n_s, n_t - 1, rows, tokens), bf16),
        V((n_t - 1, rest, tokens), bf16),
        V((max(n_s - 2, 1), rows, tokens), bf16),
        V((n_t, early, tokens), bf16),
        V((rest, tokens), bf16),
    ]
    parts = 6 if width % (6 * 128) == 0 else 1
    div, gw, gh = pl.pallas_call(
        functools.partial(kernel, n_t, n_s, blk),
        out_shape=(
            jax.ShapeDtypeStruct((1, tokens), f32),
            jax.ShapeDtypeStruct((half, shard), bf16),
            jax.ShapeDtypeStruct((rows, tokens), f32),
        ),
        in_specs=[hbm] * 6,
        out_specs=(vmem, vmem, vmem),
        scratch_shapes=[
            pltpu.SMEM((1, 1, 2, slots), jnp.int32),
            pltpu.SMEM((1, 1), jnp.int32),
            V((teacher_probs.shape[1] // blk, tokens, blk), bf16),
            V(block_values.shape[2:], bf16),
            V(hidden.shape, bf16),
            V(student_weight.shape, bf16),
            V((tokens, half), bf16),
            V((half, 2 * tokens), bf16),
            V((slots + 1, tokens, blk), f32),
            V((slots, lanes), f32),
            V((1, tokens), f32),
            V((2, lanes), jnp.int32),
            pltpu.SMEM((2, lanes), jnp.int32),
            V(parcel, bf16),
            V(parcel, bf16),
            V((tokens, shard), f32),
            V((tokens, shard), f32),
            V((tokens, shard), f32),
            V((tokens, 128), f32),
            V((n, 4, tokens), f32),
            V((n, 2, tokens), f32),
            V((2 * tokens, shard), bf16),
            V((shard, tokens), bf16),
            V((8, 128) if direct else (width, tokens), f32),
            *exchange,
            DMA((6,)), DMA((parts,)), DMA((4,)), DMA, DMA((n_t,)), DMA((2,)), DMA((3,)),
            DMA((3,)), DMA((n_s,)), DMA, DMA, DMA,
        ],
        compiler_params=pltpu.CompilerParams(
            collective_id=0, has_side_effects=True, vmem_limit_bytes=32 * 1024 * 1024),
    )(
        pltpu.with_memory_space_constraint(jnp.swapaxes(block_index, 2, 3), pltpu.HBM), block_count,
        *(pltpu.with_memory_space_constraint(x, pltpu.HBM) for x in (teacher_probs, block_values, hidden, student_weight)))
    div, gw, gh = pl.pallas_call(
        flush,
        out_shape=tuple(jax.ShapeDtypeStruct(x.shape, x.dtype) for x in (div, gw, gh)),
        in_specs=[vmem] * 3,
        out_specs=(hbm,) * 3,
        scratch_shapes=[DMA((3,))],
        compiler_params=pltpu.CompilerParams(vmem_limit_bytes=2**20),
    )(div, gw, gh)
    return div.reshape(tokens), gw, gh.T


def solution(mesh):
    return jax.shard_map(
        functools.partial(local, mesh.shape["tvoc"], mesh.shape["svoc"]),
        mesh=mesh,
        in_specs=(
            P("dp", "tvoc"),
            P("tvoc", "svoc", None, None, None),
            P("tvoc", "svoc", None, None),
            P("tvoc", "svoc"),
            P("dp", None),
            P(None, ("tvoc", "svoc")),
        ),
        out_specs=(P("dp"), P("dp", ("tvoc", "svoc")), P("dp", ("tvoc", "svoc"))),
        check_vma=False,
    )
```
